256 devices in a mesh: px: 4 (over z_hi), py: 8 (over z_lo, y), sa: 8 (over x, core).
Axes of the slice: x: 4, y: 4, z: 8 (z_hi: 4, z_lo: 2; z = z_hi * 2 + z_lo), core: 2. Of those that a mesh axis runs over, the one named last changes fastest.
Arguments:
- real_coeffs: float32 [8, 256, 256, 256], P('sa', 'px', 'py'), may hold values from -6 to 6
- imaginary_coeffs: float32 [8, 256, 256, 256], P('sa', 'px', 'py'), may hold values from -6 to 6
Outputs:
- modulus: float32 [8, 256, 256, 256], P(None, ('px', 'py'), 'sa')
The draws below stay inside these ranges and needn't reach their ends.
All inputs are finite; a program needn't handle non-finite values.
Results may differ from the reference program's by a relative error of at most 0.00007.
Values sent between devices are 32-bit elements; how exact they have to be, the bound alone decides.
A program may use at most 64 MiB of HBM per device.

```python
import math
import jax
import jax.numpy as jnp
from jax import lax

N = 256
SAMPLES = 8


def steps_of(stream_key, extent, pieces, smallest, top_value):
    loudness, own = 1.0, jax.random.fold_in(stream_key, 6)
    for dim, shards_of in pieces:
        steps = jnp.exp(jax.random.uniform(jax.random.fold_in(own, dim), (shards_of,), jnp.float32, smallest / len(pieces), top_value / len(pieces)))
        loudness = loudness * jnp.repeat(steps, extent[dim] // shards_of).reshape([-1 if axis == dim else 1 for axis in range(len(extent))])
    return loudness


def centred(rng, dims, scale, most, cuts=(), held_as=jnp.bfloat16):
    values = jax.random.normal(rng, dims, jnp.float32) * scale
    if len(cuts) > 0:
        values = steps_of(rng, dims, cuts, -0.22, 0.18) * values
    return jnp.clip(values, min=-most, max=most).astype(held_as)


def setup_inputs(seed: int = 0) -> dict:
    key_of = jax.random.split(jax.random.key(seed), 3)
    return {
        "real_coeffs": centred(key_of[0], (SAMPLES, N, N, N), 1.0, 6.0, ((0, 8), (1, 4), (2, 8)), jnp.float32),
        "imaginary_coeffs": centred(key_of[1], (SAMPLES, N, N, N), 1.0, 6.0, ((0, 8), (1, 4), (2, 8)), jnp.float32),
    }


corr_length = 1.0
log_spread = 0.5

def matern(squared, length):
    return 1.0 / (1.0 + (2.0 * math.pi * corr_length / length) ** 2 * squared)

def matern_scale(length):
    middle = length // 2
    square_counts = {}
    for position in range(length):
        square_value = ((position + middle) % length - middle) ** 2
        square_counts[square_value] = square_counts.get(square_value, 0) + 1
    plane_counts = {}
    for first_square, first_count in square_counts.items():
        for second_square, second_count in square_counts.items():
            plane_sum = first_square + second_square
            plane_counts[plane_sum] = plane_counts.get(plane_sum, 0) + first_count * second_count
    running = 0.0
    for first_square, first_count in square_counts.items():
        for plane_sum, plane_count in plane_counts.items():
            running = running + first_count * plane_count * matern(first_square + plane_sum, length) ** 2
    return 1.0 / math.sqrt(running)

def reference(real_coeffs, imaginary_coeffs):
    frequency = ((jnp.arange(N, dtype=jnp.int32) + N // 2) % N - N // 2).astype(jnp.float32)
    squared = frequency[:, None, None] ** 2 + frequency[None, :, None] ** 2 + frequency[None, None, :] ** 2
    weight = matern(squared, N) * matern_scale(N)

    def one_sample(coeff_pair):
        real_part = jnp.transpose(coeff_pair[0], (2, 0, 1))
        imag_part = jnp.transpose(coeff_pair[1], (2, 0, 1))
        spectrum = lax.complex(weight * real_part, weight * imag_part)
        log_field = jnp.real(jnp.fft.ifftn(spectrum)) * float(N ** 3)
        return jnp.exp(log_spread * log_field).astype(jnp.float32)
    return lax.map(one_sample, (real_coeffs, imaginary_coeffs))
```

```python
import math

import jax
import jax.numpy as jnp
import numpy as np
from jax import lax
from jax.experimental import pallas as pl
from jax.experimental.pallas import tpu as pltpu
from jax.sharding import PartitionSpec as P

MESH = pl.DeviceIdType.MESH
corr_length = 1.0
log_spread = 0.5

N = 256
GROUP = 32
CHUNKS = 8
PITCH = 40


def matern(squared, length):
    return 1.0 / (1.0 + (2.0 * math.pi * corr_length / length) ** 2 * squared)


def matern_scale(length):
    middle = length // 2
    square_counts = {}
    for position in range(length):
        square_value = ((position + middle) % length - middle) ** 2
        square_counts[square_value] = square_counts.get(square_value, 0) + 1
    plane_counts = {}
    for first_square, first_count in square_counts.items():
        for second_square, second_count in square_counts.items():
            plane_sum = first_square + second_square
            plane_counts[plane_sum] = plane_counts.get(plane_sum, 0) + first_count * second_count
    running = 0.0
    for first_square, first_count in square_counts.items():
        for plane_sum, plane_count in plane_counts.items():
            running = (
                running + first_count * plane_count * matern(first_square + plane_sum, length) ** 2
            )
    return 1.0 / math.sqrt(running)


def halves(table):
    high = table.astype(np.float32).astype(jnp.bfloat16)
    low = (table - high.astype(np.float64)).astype(np.float32).astype(jnp.bfloat16)
    return high, low


def phases(rows, columns):
    angles = (np.asarray(rows)[:, None] * np.asarray(columns)[None, :] % N) * (2.0 * np.pi / N)
    return np.cos(angles), np.sin(angles)


def x_table():
    pieces = []
    for j in range(CHUNKS):
        cos, sin = phases(np.arange(GROUP) * CHUNKS + j, np.arange(N))
        pieces.append(np.block([[cos, -sin], [sin, cos]]))
    high, low = halves(np.stack(pieces))
    return np.concatenate([high, low], axis=1)


def z_table():
    odd, owner, pair = np.meshgrid(np.arange(2), np.arange(8), np.arange(16), indexing="ij")
    waves = (owner * 32 + pair * 2 + odd).reshape(-1)
    cos, sin = phases(np.arange(N), waves)
    high, low = halves(np.block([[cos, -sin], [sin, cos]]))
    return np.concatenate([high, low], axis=0)


def y_table():
    cos, sin = phases(np.arange(N), np.arange(N))
    high, low = halves(np.concatenate([cos, -sin], axis=1))
    return np.concatenate([high, low], axis=0)


def split(value):
    high = value.astype(jnp.bfloat16)
    low = (value - high.astype(jnp.float32)).astype(jnp.bfloat16)
    return high, low


def dot(left, right, transposed):
    return lax.dot_general(
        left,
        right,
        (((1,), (1 if transposed else 0,)), ((), ())),
        preferred_element_type=jnp.float32,
    )


def signed(positions):
    return ((positions + N // 2) % N - N // 2).astype(jnp.float32)


def kernel(
    re_hbm, im_hbm, tx_hbm, tz_hbm, ty_hbm, out_ref,
    xbuf, dhigh, dlow, gbuf, rbuf, obuf, tx, tz, ty, whigh, wlow, bhigh, blow,
    in_sem, table_sem, send_sem, recv_sem, out_send_sem, out_recv_sem,
):
    px, py, sa = lax.axis_index("px"), lax.axis_index("py"), lax.axis_index("sa")
    me = px * 8 + py
    z, y = px * 2 + py // 4, py % 4

    def plane_peer(dz, dy):
        z2, y2 = (z + dz) % 8, (y + dy) % 4
        return z2 // 2, (z2 % 2) * 4 + y2

    order = (4, 3, -3, 2, -2, 1, -1, 0)
    offsets = [(dz, dy) for dz in order for dy in range(4) if (dz, dy) != (0, 0)]

    barrier = pltpu.get_barrier_semaphore()
    for dz, dy in offsets:
        p, q = plane_peer(dz, dy)
        pl.semaphore_signal(barrier, inc=1, device_id={"px": p, "py": q}, device_id_type=MESH)
    for step in range(1, 8):
        pl.semaphore_signal(
            barrier, inc=1, device_id={"sa": (sa + step) % 8}, device_id_type=MESH
        )

    table_copies = [
        pltpu.make_async_copy(tx_hbm, tx, table_sem.at[0]),
        pltpu.make_async_copy(tz_hbm, tz, table_sem.at[1]),
        pltpu.make_async_copy(ty_hbm, ty, table_sem.at[2]),
    ]
    in_copies = []
    for block in range(4):
        group = []
        for part, source in enumerate((re_hbm, im_hbm)):
            for half in range(2):
                copy = pltpu.make_async_copy(
                    source.at[0, :, pl.ds(block * 8, 8), pl.ds(half * 128, 128)],
                    xbuf.at[part * 2 + half, :, pl.ds(block * 8, 8), :],
                    in_sem.at[block, part * 2 + half],
                )
                copy.start()
                group.append(copy)
        in_copies.append(group)
        if block == 0:
            table_copies[0].start()
    table_copies[1].start()
    table_copies[2].start()

    scale = matern_scale(N)
    slope = (2.0 * math.pi * corr_length / N) ** 2
    fy = signed(lax.broadcasted_iota(jnp.int32, (64, 128), 0) + px * 64) ** 2
    lanes = lax.broadcasted_iota(jnp.int32, (64, 128), 1)
    flat = signed(lanes) ** 2 + fy, signed(lanes + 128) ** 2 + fy
    lines = xbuf.reshape(4, 64 * PITCH, 128)

    for block in range(4):
        for copy in in_copies[block]:
            copy.wait()

        def weigh(step, carry, block=block):
            k = block * 8 + step
            fz = signed(py * 32 + k) ** 2
            rows = pl.ds(pl.multiple_of(k * 64, 64), 64)
            for half in range(2):
                weight = (1.0 / (1.0 + slope * (flat[half] + fz))) * scale
                for part in range(2):
                    value = lines[part * 2 + half, pl.ds(k, 64, stride=PITCH), :] * weight
                    high, low = split(value)
                    columns = pl.ds(part * N + half * 128, 128)
                    dhigh[rows, columns] = high
                    dlow[rows, columns] = low
            return carry

        lax.fori_loop(0, 8, weigh, 0)
    table_copies[0].wait()

    pl.semaphore_wait(barrier, len(offsets) + 7)

    def message(j, d):
        return gbuf.at[pl.ds(pl.multiple_of((j * GROUP + d) * PITCH, 8), 32), :]

    def forward(j, carry):
        base = j * (GROUP * PITCH)
        for block in range(8):
            rows = pl.ds(block * 256, 256)
            both = dot(tx[j], dhigh[rows, :], True)
            piece = both[:64] + both[64:] + dot(tx[j, :64], dlow[rows, :], True)
            for part in range(2):
                for half in range(2):
                    at = base + part * 16 + block * 2 + half
                    gbuf[pl.ds(at, GROUP, stride=PITCH), :] = piece[
                        part * 32 : part * 32 + 32, half * 128 : half * 128 + 128
                    ]
        for dz, dy in offsets:
            p, q = plane_peer(dz, dy)
            pltpu.make_async_remote_copy(
                src_ref=message(j, p * 8 + q),
                dst_ref=rbuf.at[j, me],
                send_sem=send_sem.at[j],
                recv_sem=recv_sem.at[j],
                device_id={"px": p, "py": q},
                device_id_type=MESH,
            ).start()
        rbuf[j, me] = gbuf[pl.ds(pl.multiple_of((j * GROUP + me) * PITCH, 8), 32), :]
        return carry

    lax.fori_loop(0, CHUNKS, forward, 0)
    table_copies[1].wait()
    table_copies[2].wait()

    low_lanes = lax.broadcasted_iota(jnp.int32, (128, 128), 1) < 64

    def finish(j, carry):
        arrived = rbuf.at[j, pl.ds(0, GROUP - 1)]
        pltpu.make_async_copy(arrived, arrived, recv_sem.at[j]).wait()
        for part in range(2):
            for pair in range(2):
                first, second = (
                    rbuf[
                        j, pl.ds((pair * 2 + k) * 8, 8), pl.ds(part * 16, 16), :
                    ].reshape(128, 128)
                    for k in range(2)
                )
                even = jnp.where(low_lanes, first, pltpu.roll(second, 64, 1))
                odd = jnp.where(low_lanes, pltpu.roll(first, 64, 1), second)
                for k, value in enumerate((even, odd)):
                    rows = pl.ds(part * N + k * 128, 128)
                    columns = pl.ds(pair * 128, 128)
                    high, low = split(value)
                    bhigh[rows, columns] = high
                    blow[rows, columns] = low
        both = dot(tz[...], bhigh[...], False)
        partial = both[:512] + both[512:] + dot(tz[:512], blow[...], False)
        for part in range(2):
            high, low = split(partial[part * N : part * N + N])
            whigh[:, pl.ds(part * N, N)] = high
            wlow[:, pl.ds(part * N, N)] = low
        both = dot(ty[...], whigh[...], True)
        field = both[:N] + both[N:] + dot(ty[:N], wlow[...], True)
        obuf[j] = jnp.exp(log_spread * field)
        for step in range(1, 8):
            other = (sa + step) % 8
            pltpu.make_async_remote_copy(
                src_ref=obuf.at[j, pl.ds(pl.multiple_of(other * 32, 32), 32), :],
                dst_ref=out_ref.at[sa, j],
                send_sem=out_send_sem.at[j],
                recv_sem=out_recv_sem.at[j],
                device_id={"sa": other},
                device_id_type=MESH,
            ).start()
        out_ref[sa, j] = obuf[j, pl.ds(pl.multiple_of(sa * 32, 32), 32), :]
        return carry

    lax.fori_loop(0, CHUNKS, finish, 0)

    def drain(j, carry):
        sent = rbuf.at[j, pl.ds(0, GROUP - 1)]
        pltpu.make_async_copy(sent, sent, send_sem.at[j]).wait()
        moved = obuf.at[j, pl.ds(0, 7 * 32), :]
        pltpu.make_async_copy(moved, moved, out_send_sem.at[j]).wait()
        pltpu.make_async_copy(moved, moved, out_recv_sem.at[j]).wait()
        return carry

    lax.fori_loop(0, CHUNKS, drain, 0)


def local(real_coeffs, imaginary_coeffs):
    anywhere = pl.BlockSpec(memory_space=pl.ANY)
    return pl.pallas_call(
        kernel,
        out_shape=jax.ShapeDtypeStruct((8, CHUNKS, 32, N), jnp.float32),
        in_specs=[anywhere] * 5,
        out_specs=pl.BlockSpec(memory_space=pltpu.VMEM),
        scratch_shapes=[
            pltpu.VMEM((4, 64, PITCH, 128), jnp.float32),
            pltpu.VMEM((2048, 512), jnp.bfloat16),
            pltpu.VMEM((2048, 512), jnp.bfloat16),
            pltpu.VMEM((CHUNKS * GROUP * PITCH, 128), jnp.float32),
            pltpu.VMEM((CHUNKS, GROUP, 32, 128), jnp.float32),
            pltpu.VMEM((CHUNKS, N, N), jnp.float32),
            pltpu.VMEM((CHUNKS, 128, 512), jnp.bfloat16),
            pltpu.VMEM((1024, 512), jnp.bfloat16),
            pltpu.VMEM((512, 512), jnp.bfloat16),
            pltpu.VMEM((N, 512), jnp.bfloat16),
            pltpu.VMEM((N, 512), jnp.bfloat16),
            pltpu.VMEM((512, N), jnp.bfloat16),
            pltpu.VMEM((512, N), jnp.bfloat16),
            pltpu.SemaphoreType.DMA((4, 4)),
            pltpu.SemaphoreType.DMA((3,)),
            pltpu.SemaphoreType.DMA((CHUNKS,)),
            pltpu.SemaphoreType.DMA((CHUNKS,)),
            pltpu.SemaphoreType.DMA((CHUNKS,)),
            pltpu.SemaphoreType.DMA((CHUNKS,)),
        ],
        compiler_params=pltpu.CompilerParams(
            collective_id=0, has_side_effects=True, vmem_limit_bytes=56 * 1024 * 1024
        ),
    )(real_coeffs, imaginary_coeffs, x_table(), z_table(), y_table())


def solution(mesh):
    placed = (P("sa", "px", "py", None), P("sa", "px", "py", None))
    return jax.shard_map(
        local,
        mesh=mesh,
        in_specs=placed,
        out_specs=P(None, ("px", "py"), "sa", None),
        check_vma=False,
    )
```

```python
import math

import jax
import jax.numpy as jnp
import numpy as np
from jax import lax
from jax.experimental import pallas as pl
from jax.experimental.pallas import tpu as pltpu
from jax.sharding import PartitionSpec as P

MESH = pl.DeviceIdType.MESH
corr_length = 1.0
log_spread = 0.5

N = 256
GROUP = 32
CHUNKS = 8
PITCH = 40


def matern(squared, length):
    return 1.0 / (1.0 + (2.0 * math.pi * corr_length / length) ** 2 * squared)


def matern_scale(length):
    middle = length // 2
    square_counts = {}
    for position in range(length):
        square_value = ((position + middle) % length - middle) ** 2
        square_counts[square_value] = square_counts.get(square_value, 0) + 1
    plane_counts = {}
    for first_square, first_count in square_counts.items():
        for second_square, second_count in square_counts.items():
            plane_sum = first_square + second_square
            plane_counts[plane_sum] = plane_counts.get(plane_sum, 0) + first_count * second_count
    running = 0.0
    for first_square, first_count in square_counts.items():
        for plane_sum, plane_count in plane_counts.items():
            running = (
                running + first_count * plane_count * matern(first_square + plane_sum, length) ** 2
            )
    return 1.0 / math.sqrt(running)


def halves(table):
    high = table.astype(np.float32).astype(jnp.bfloat16)
    low = (table - high.astype(np.float64)).astype(np.float32).astype(jnp.bfloat16)
    return high, low


def phases(rows, columns):
    angles = (np.asarray(rows)[:, None] * np.asarray(columns)[None, :] % N) * (2.0 * np.pi / N)
    return np.cos(angles), np.sin(angles)


def x_table():
    pieces = []
    for j in range(CHUNKS):
        cos, sin = phases(np.arange(GROUP) * CHUNKS + j, np.arange(N))
        pieces.append(np.block([[cos, -sin], [sin, cos]]))
    high, low = halves(np.stack(pieces))
    return np.concatenate([high, low], axis=1).reshape(-1, 2 * N)


def z_table():
    odd, owner, block, part, row = np.meshgrid(
        *(np.arange(n) for n in (2, 8, 4, 2, 4)), indexing="ij"
    )
    waves = (owner * 32 + (block * 4 + row) * 2 + odd).reshape(-1)
    real = part.reshape(-1)[None, :] == 0
    cos, sin = phases(np.arange(N), waves)
    high, low = halves(np.concatenate([np.where(real, cos, -sin), np.where(real, sin, cos)]))
    return np.concatenate([high, low], axis=0)


def y_table():
    cos, sin = phases(np.arange(N), np.arange(N))
    high, low = halves(np.concatenate([cos, -sin], axis=1))
    return np.concatenate([high, low], axis=0)


def split(value):
    high = value.astype(jnp.bfloat16)
    low = (value - high.astype(jnp.float32)).astype(jnp.bfloat16)
    return high, low


def dot(left, right, transposed):
    return lax.dot_general(
        left,
        right,
        (((1,), (1 if transposed else 0,)), ((), ())),
        preferred_element_type=jnp.float32,
    )


def signed(positions):
    return ((positions + N // 2) % N - N // 2).astype(jnp.float32)


def kernel(
    re_hbm, im_hbm, tables_hbm, out_ref,
    xbuf, dhigh, dlow, gbuf, rbuf, obuf, tx, tz, ty, whigh, wlow, bhigh, blow,
    in_sem, table_sem, send_sem, recv_sem, out_send_sem, out_recv_sem,
):
    px, py, sa = lax.axis_index("px"), lax.axis_index("py"), lax.axis_index("sa")
    me = px * 8 + py
    z, y = px * 2 + lax.div(py, 4), lax.rem(py, 4)

    in_copies = []
    for block in range(4):
        group = []
        for part, source in enumerate((re_hbm, im_hbm)):
            for half in range(2):
                group.append(
                    pltpu.make_async_copy(
                        source.at[0, :, pl.ds(block * 8, 8), pl.ds(half * 128, 128)],
                        xbuf.at[part * 2 + half, :, pl.ds(block * 8, 8), :],
                        in_sem.at[block, part * 2 + half],
                    )
                )
        in_copies.append(group)
    table_copies = [
        pltpu.make_async_copy(
            tables_hbm.at[pl.ds(start, size), :], target.at[pl.ds(at, size), :], table_sem.at[i]
        )
        for i, (start, size, target, at) in enumerate(
            ((0, 128, tx, 0), (128, 896, tx, 128), (1024, 1024, tz, 0), (2048, 512, ty, 0))
        )
    ]
    for copy in in_copies[0]:
        copy.start()
    table_copies[0].start()

    def plane_peer(dz, dy):
        z2, y2 = lax.rem(z + (dz + 8) % 8, 8), lax.rem(y + dy, 4)
        return lax.div(z2, 2), lax.rem(z2, 2) * 4 + y2

    order = (4, 3, -3, 2, -2, 1, -1, 0)
    peers = [plane_peer(dz, dy) for dz in order for dy in range(4) if (dz, dy) != (0, 0)]
    others = [lax.rem(sa + step, 8) for step in range(1, 8)]

    barrier = pltpu.get_barrier_semaphore()
    for p, q in peers:
        pl.semaphore_signal(barrier, inc=1, device_id={"px": p, "py": q}, device_id_type=MESH)
    for other in others:
        pl.semaphore_signal(barrier, inc=1, device_id={"sa": other}, device_id_type=MESH)

    for group in in_copies[1:]:
        for copy in group:
            copy.start()
    for copy in table_copies[1:]:
        copy.start()

    scale = matern_scale(N)
    slope = (2.0 * math.pi * corr_length / N) ** 2
    fy = signed(lax.broadcasted_iota(jnp.int32, (64, 128), 0) + px * 64) ** 2
    lanes = lax.broadcasted_iota(jnp.int32, (64, 128), 1)
    flat = signed(lanes) ** 2 + fy, signed(lanes + 128) ** 2 + fy
    lines = xbuf.reshape(4, 64 * PITCH, 128)

    def weigh(k, carry):
        fz = signed(py * 32 + k) ** 2
        rows = pl.ds(pl.multiple_of(k * 64, 64), 64)
        for half in range(2):
            weight = (1.0 / (1.0 + slope * (flat[half] + fz))) * scale
            for part in range(2):
                value = lines[part * 2 + half, pl.ds(k, 64, stride=PITCH), :] * weight
                high, low = split(value)
                columns = pl.ds(part * N + half * 128, 128)
                dhigh[rows, columns] = high
                dlow[rows, columns] = low
        return carry

    def transform(j, block):
        base = j * (GROUP * PITCH)
        table = pl.multiple_of(j * 128, 128)
        for piece in range(2):
            rows = pl.ds(block * 512 + piece * 256, 256)
            both = dot(tx[pl.ds(table, 128), :], dhigh[rows, :], True)
            result = both[:64] + both[64:] + dot(tx[pl.ds(table, 64), :], dlow[rows, :], True)
            for part in range(2):
                for half in range(2):
                    at = base + block * 8 + part * 4 + piece * 2 + half
                    gbuf[pl.ds(at, GROUP, stride=PITCH), :] = result[
                        part * 32 : part * 32 + 32, half * 128 : half * 128 + 128
                    ]

    def send(j, first, count):
        for p, q in peers:
            row = pl.multiple_of((j * GROUP + p * 8 + q) * PITCH + first, 8)
            pltpu.make_async_remote_copy(
                src_ref=gbuf.at[pl.ds(row, count), :],
                dst_ref=rbuf.at[j, me, pl.ds(first, count), :],
                send_sem=send_sem.at[j],
                recv_sem=recv_sem.at[j],
                device_id={"px": p, "py": q},
                device_id_type=MESH,
            ).start()

    def keep(j):
        rbuf[j, me] = gbuf[pl.ds(pl.multiple_of((j * GROUP + me) * PITCH, 8), 32), :]

    for block in range(4):
        for copy in in_copies[block]:
            copy.wait()
        lax.fori_loop(block * 8, block * 8 + 8, weigh, 0)
        if block == 0:
            table_copies[0].wait()
        transform(0, block)
        if block == 0:
            pl.semaphore_wait(barrier, len(peers) + len(others))
        send(0, block * 8, 8)
    keep(0)
    table_copies[1].wait()

    def forward(j, carry):
        for block in range(4):
            transform(j, block)
        send(j, 0, 32)
        keep(j)
        return carry

    lax.fori_loop(1, CHUNKS, forward, 0)
    table_copies[2].wait()
    table_copies[3].wait()

    low_lanes = lax.broadcasted_iota(jnp.int32, (N, 128), 1) < 64

    def finish(j, carry):
        arrived = rbuf.at[j, pl.ds(0, GROUP - 1)]
        pltpu.make_async_copy(arrived, arrived, recv_sem.at[j]).wait()
        for pair in range(2):
            first, second = (
                rbuf[j, pl.ds((pair * 2 + k) * 8, 8)].reshape(N, 128) for k in range(2)
            )
            even = jnp.where(low_lanes, first, pltpu.roll(second, 64, 1))
            odd = jnp.where(low_lanes, pltpu.roll(first, 64, 1), second)
            for k, value in enumerate((even, odd)):
                rows = pl.ds(k * N, N)
                columns = pl.ds(pair * 128, 128)
                high, low = split(value)
                bhigh[rows, columns] = high
                blow[rows, columns] = low
        both = dot(tz[...], bhigh[...], False)
        partial = both[:512] + both[512:] + dot(tz[:512], blow[...], False)
        for part in range(2):
            high, low = split(partial[part * N : part * N + N])
            whigh[:, pl.ds(part * N, N)] = high
            wlow[:, pl.ds(part * N, N)] = low
        both = dot(ty[...], whigh[...], True)
        field = both[:N] + both[N:] + dot(ty[:N], wlow[...], True)
        obuf[j] = jnp.exp(log_spread * field)
        for other in others:
            pltpu.make_async_remote_copy(
                src_ref=obuf.at[j, pl.ds(pl.multiple_of(other * 32, 32), 32), :],
                dst_ref=out_ref.at[sa, j],
                send_sem=out_send_sem.at[j],
                recv_sem=out_recv_sem.at[j],
                device_id={"sa": other},
                device_id_type=MESH,
            ).start()
        out_ref[sa, j] = obuf[j, pl.ds(pl.multiple_of(sa * 32, 32), 32), :]
        return carry

    lax.fori_loop(0, CHUNKS, finish, 0)

    def drain(j, carry):
        sent = rbuf.at[j, pl.ds(0, GROUP - 1)]
        pltpu.make_async_copy(sent, sent, send_sem.at[j]).wait()
        moved = obuf.at[j, pl.ds(0, 7 * 32), :]
        pltpu.make_async_copy(moved, moved, out_send_sem.at[j]).wait()
        pltpu.make_async_copy(moved, moved, out_recv_sem.at[j]).wait()
        return carry

    lax.fori_loop(0, CHUNKS, drain, 0)


def local(real_coeffs, imaginary_coeffs):
    anywhere = pl.BlockSpec(memory_space=pltpu.HBM)
    return pl.pallas_call(
        kernel,
        out_shape=jax.ShapeDtypeStruct((8, CHUNKS, 32, N), jnp.float32),
        in_specs=[anywhere] * 3,
        out_specs=pl.BlockSpec(memory_space=pltpu.VMEM),
        scratch_shapes=[
            pltpu.VMEM((4, 64, PITCH, 128), jnp.float32),
            pltpu.VMEM((2048, 512), jnp.bfloat16),
            pltpu.VMEM((2048, 512), jnp.bfloat16),
            pltpu.VMEM((CHUNKS * GROUP * PITCH, 128), jnp.float32),
            pltpu.VMEM((CHUNKS, GROUP, 32, 128), jnp.float32),
            pltpu.VMEM((CHUNKS, N, N), jnp.float32),
            pltpu.VMEM((CHUNKS * 128, 512), jnp.bfloat16),
            pltpu.VMEM((1024, 512), jnp.bfloat16),
            pltpu.VMEM((512, 512), jnp.bfloat16),
            pltpu.VMEM((N, 512), jnp.bfloat16),
            pltpu.VMEM((N, 512), jnp.bfloat16),
            pltpu.VMEM((512, N), jnp.bfloat16),
            pltpu.VMEM((512, N), jnp.bfloat16),
            pltpu.SemaphoreType.DMA((4, 4)),
            pltpu.SemaphoreType.DMA((4,)),
            pltpu.SemaphoreType.DMA((CHUNKS,)),
            pltpu.SemaphoreType.DMA((CHUNKS,)),
            pltpu.SemaphoreType.DMA((CHUNKS,)),
            pltpu.SemaphoreType.DMA((CHUNKS,)),
        ],
        compiler_params=pltpu.CompilerParams(
            collective_id=0, has_side_effects=True, vmem_limit_bytes=50 * 1024 * 1024
        ),
    )(real_coeffs, imaginary_coeffs, np.concatenate([x_table(), z_table(), y_table()]))


def solution(mesh):
    placed = (P("sa", "px", "py", None), P("sa", "px", "py", None))
    return jax.shard_map(
        local,
        mesh=mesh,
        in_specs=placed,
        out_specs=P(None, ("px", "py"), "sa", None),
        check_vma=False,
    )
```

```python
import math

import jax
import jax.numpy as jnp
import numpy as np
from jax import lax
from jax.experimental import pallas as pl
from jax.experimental.pallas import tpu as pltpu
from jax.sharding import PartitionSpec as P

MESH = pl.DeviceIdType.MESH
corr_length = 1.0
log_spread = 0.5

N = 256
GROUP = 32
CHUNKS = 8
PITCH = 40


def matern(squared, length):
    return 1.0 / (1.0 + (2.0 * math.pi * corr_length / length) ** 2 * squared)


def matern_scale(length):
    middle = length // 2
    square_counts = {}
    for position in range(length):
        square_value = ((position + middle) % length - middle) ** 2
        square_counts[square_value] = square_counts.get(square_value, 0) + 1
    plane_counts = {}
    for first_square, first_count in square_counts.items():
        for second_square, second_count in square_counts.items():
            plane_sum = first_square + second_square
            plane_counts[plane_sum] = plane_counts.get(plane_sum, 0) + first_count * second_count
    running = 0.0
    for first_square, first_count in square_counts.items():
        for plane_sum, plane_count in plane_counts.items():
            running = (
                running + first_count * plane_count * matern(first_square + plane_sum, length) ** 2
            )
    return 1.0 / math.sqrt(running)


def halves(table):
    high = table.astype(np.float32).astype(jnp.bfloat16)
    low = (table - high.astype(np.float64)).astype(np.float32).astype(jnp.bfloat16)
    return high, low


def phases(rows, columns):
    angles = (np.asarray(rows)[:, None] * np.asarray(columns)[None, :] % N) * (2.0 * np.pi / N)
    return np.cos(angles), np.sin(angles)


def x_table():
    pieces = []
    for j in range(CHUNKS):
        cos, sin = phases(np.arange(GROUP) * CHUNKS + j, np.arange(N))
        pieces.append(np.block([[cos, -sin], [sin, cos]]))
    high, low = halves(np.stack(pieces))
    return np.concatenate([high, low], axis=1).reshape(-1, 2 * N)


def z_table():
    odd, owner, block, part, row = np.meshgrid(
        *(np.arange(n) for n in (2, 8, 4, 2, 4)), indexing="ij"
    )
    waves = (owner * 32 + (block * 4 + row) * 2 + odd).reshape(-1)
    real = part.reshape(-1)[None, :] == 0
    cos, sin = phases(np.arange(N), waves)
    high, low = halves(np.concatenate([np.where(real, cos, -sin), np.where(real, sin, cos)]))
    return np.concatenate([high, low], axis=0)


def y_table():
    cos, sin = phases(np.arange(N), np.arange(N))
    high, low = halves(np.concatenate([cos, -sin], axis=1))
    return np.concatenate([high, low], axis=0)


def split(value):
    high = value.astype(jnp.bfloat16)
    low = (value - high.astype(jnp.float32)).astype(jnp.bfloat16)
    return high, low


def dot(left, right, transposed):
    return lax.dot_general(
        left,
        right,
        (((1,), (1 if transposed else 0,)), ((), ())),
        preferred_element_type=jnp.float32,
    )


def signed(positions):
    return ((positions + N // 2) % N - N // 2).astype(jnp.float32)


def kernel(
    re_hbm, im_hbm, tables_hbm, out_ref,
    xbuf, dhigh, dlow, gbuf, rbuf, obuf, tx, tz, ty, whigh, wlow, bhigh, blow,
    in_sem, table_sem, send_sem, recv_sem, out_send_sem, out_recv_sem, ready_sem,
):
    px, py, sa = lax.axis_index("px"), lax.axis_index("py"), lax.axis_index("sa")
    me = px * 8 + py
    z, y = px * 2 + lax.div(py, 4), lax.rem(py, 4)

    in_copies = []
    for block in range(4):
        group = []
        for part, source in enumerate((re_hbm, im_hbm)):
            for half in range(2):
                group.append(
                    pltpu.make_async_copy(
                        source.at[0, :, pl.ds(block * 8, 8), pl.ds(half * 128, 128)],
                        xbuf.at[part * 2 + half, :, pl.ds(block * 8, 8), :],
                        in_sem.at[block, part * 2 + half],
                    )
                )
        in_copies.append(group)
    table_copies = [
        pltpu.make_async_copy(
            tables_hbm.at[pl.ds(start, size), :], target.at[pl.ds(at, size), :], table_sem.at[i]
        )
        for i, (start, size, target, at) in enumerate(
            ((0, 128, tx, 0), (128, 896, tx, 128), (1024, 1024, tz, 0), (2048, 512, ty, 0))
        )
    ]
    for copy in in_copies[0]:
        copy.start()
    table_copies[0].start()

    def plane_peer(dz, dy):
        z2, y2 = lax.rem(z + (dz + 8) % 8, 8), lax.rem(y + dy, 4)
        return lax.div(z2, 2), lax.rem(z2, 2) * 4 + y2

    near, two, three, four = (
        [plane_peer(dz, dy) for dz in dzs for dy in range(4) if (dz, dy) != (0, 0)]
        for dzs in ((1, -1, 0), (2, -2), (3, -3), (4,))
    )
    peers = four + three + two + near
    beside = [plane_peer(1, 0), plane_peer(-1, 0)]
    x, core = lax.div(sa, 2), lax.rem(sa, 2)
    others = [
        lax.rem(x + dx, 4) * 2 + lax.rem(core + dc, 2)
        for dx in (2, 1, 3, 0)
        for dc in range(2)
        if (dx, dc) != (0, 0)
    ]

    barrier = pltpu.get_barrier_semaphore()
    for p, q in near:
        pl.semaphore_signal(barrier, inc=1, device_id={"px": p, "py": q}, device_id_type=MESH)
    for other in others:
        pl.semaphore_signal(barrier, inc=1, device_id={"sa": other}, device_id_type=MESH)

    def tell(level):
        for p, q in beside:
            pl.semaphore_signal(
                ready_sem.at[level], inc=1, device_id={"px": p, "py": q}, device_id_type=MESH
            )

    for group in in_copies[1:]:
        for copy in group:
            copy.start()
    for copy in table_copies[1:]:
        copy.start()

    scale = matern_scale(N)
    slope = (2.0 * math.pi * corr_length / N) ** 2
    fy = signed(lax.broadcasted_iota(jnp.int32, (64, 128), 0) + px * 64) ** 2
    lanes = lax.broadcasted_iota(jnp.int32, (64, 128), 1)
    flat = signed(lanes) ** 2 + fy, signed(lanes + 128) ** 2 + fy
    lines = xbuf.reshape(4, 64 * PITCH, 128)

    def weigh(k, carry):
        fz = signed(py * 32 + k) ** 2
        rows = pl.ds(pl.multiple_of(k * 64, 64), 64)
        for half in range(2):
            weight = (1.0 / (1.0 + slope * (flat[half] + fz))) * scale
            for part in range(2):
                value = lines[part * 2 + half, pl.ds(k, 64, stride=PITCH), :] * weight
                high, low = split(value)
                columns = pl.ds(part * N + half * 128, 128)
                dhigh[rows, columns] = high
                dlow[rows, columns] = low
        return carry

    def transform(j, block):
        base = j * (GROUP * PITCH)
        table = pl.multiple_of(j * 128, 128)
        for piece in range(2):
            rows = pl.ds(block * 512 + piece * 256, 256)
            both = dot(tx[pl.ds(table, 128), :], dhigh[rows, :], True)
            result = both[:64] + both[64:] + dot(tx[pl.ds(table, 64), :], dlow[rows, :], True)
            for part in range(2):
                for half in range(2):
                    at = base + block * 8 + part * 4 + piece * 2 + half
                    gbuf[pl.ds(at, GROUP, stride=PITCH), :] = result[
                        part * 32 : part * 32 + 32, half * 128 : half * 128 + 128
                    ]

    def send(targets, j, first, count):
        for p, q in targets:
            row = pl.multiple_of((j * GROUP + p * 8 + q) * PITCH + first, 8)
            pltpu.make_async_remote_copy(
                src_ref=gbuf.at[pl.ds(row, count), :],
                dst_ref=rbuf.at[j, me, pl.ds(first, count), :],
                send_sem=send_sem.at[j],
                recv_sem=recv_sem.at[j],
                device_id={"px": p, "py": q},
                device_id_type=MESH,
            ).start()

    def keep(j):
        rbuf[j, me] = gbuf[pl.ds(pl.multiple_of((j * GROUP + me) * PITCH, 8), 32), :]

    for block in range(4):
        for copy in in_copies[block]:
            copy.wait()
        lax.fori_loop(block * 8, block * 8 + 8, weigh, 0)
        if block == 0:
            table_copies[0].wait()
        transform(0, block)
        if block == 0:
            pl.semaphore_wait(barrier, len(near) + len(others))
        else:
            pl.semaphore_wait(ready_sem.at[block - 1], len(beside))
        if block < 3:
            tell(block)
        send((near, two, three, four)[block], 0, 0, block * 8 + 8)
        if block > 0:
            send((near, two + near, three + two + near)[block - 1], 0, block * 8, 8)
    keep(0)
    table_copies[1].wait()

    def forward(j, carry):
        for block in range(4):
            transform(j, block)
        send(peers, j, 0, 32)
        keep(j)
        return carry

    lax.fori_loop(1, CHUNKS, forward, 0)
    table_copies[2].wait()
    table_copies[3].wait()

    low_lanes = lax.broadcasted_iota(jnp.int32, (N, 128), 1) < 64

    def finish(j, carry):
        arrived = rbuf.at[j, pl.ds(0, GROUP - 1)]
        pltpu.make_async_copy(arrived, arrived, recv_sem.at[j]).wait()
        for pair in range(2):
            first, second = (
                rbuf[j, pl.ds((pair * 2 + k) * 8, 8)].reshape(N, 128) for k in range(2)
            )
            even = jnp.where(low_lanes, first, pltpu.roll(second, 64, 1))
            odd = jnp.where(low_lanes, pltpu.roll(first, 64, 1), second)
            for k, value in enumerate((even, odd)):
                rows = pl.ds(k * N, N)
                columns = pl.ds(pair * 128, 128)
                high, low = split(value)
                bhigh[rows, columns] = high
                blow[rows, columns] = low
        both = dot(tz[...], bhigh[...], False)
        partial = both[:512] + both[512:] + dot(tz[:512], blow[...], False)
        for part in range(2):
            high, low = split(partial[part * N : part * N + N])
            whigh[:, pl.ds(part * N, N)] = high
            wlow[:, pl.ds(part * N, N)] = low
        both = dot(ty[...], whigh[...], True)
        field = both[:N] + both[N:] + dot(ty[:N], wlow[...], True)
        obuf[j] = jnp.exp(log_spread * field)
        for other in others:
            pltpu.make_async_remote_copy(
                src_ref=obuf.at[j, pl.ds(pl.multiple_of(other * 32, 32), 32), :],
                dst_ref=out_ref.at[sa, j],
                send_sem=out_send_sem.at[j],
                recv_sem=out_recv_sem.at[j],
                device_id={"sa": other},
                device_id_type=MESH,
            ).start()
        out_ref[sa, j] = obuf[j, pl.ds(pl.multiple_of(sa * 32, 32), 32), :]
        return carry

    lax.fori_loop(0, CHUNKS, finish, 0)

    def drain(j, carry):
        sent = rbuf.at[j, pl.ds(0, GROUP - 1)]
        pltpu.make_async_copy(sent, sent, send_sem.at[j]).wait()
        moved = obuf.at[j, pl.ds(0, 7 * 32), :]
        pltpu.make_async_copy(moved, moved, out_send_sem.at[j]).wait()
        pltpu.make_async_copy(moved, moved, out_recv_sem.at[j]).wait()
        return carry

    lax.fori_loop(0, CHUNKS, drain, 0)


def local(real_coeffs, imaginary_coeffs):
    anywhere = pl.BlockSpec(memory_space=pltpu.HBM)
    return pl.pallas_call(
        kernel,
        out_shape=jax.ShapeDtypeStruct((8, CHUNKS, 32, N), jnp.float32),
        in_specs=[anywhere] * 3,
        out_specs=pl.BlockSpec(memory_space=pltpu.VMEM),
        scratch_shapes=[
            pltpu.VMEM((4, 64, PITCH, 128), jnp.float32),
            pltpu.VMEM((2048, 512), jnp.bfloat16),
            pltpu.VMEM((2048, 512), jnp.bfloat16),
            pltpu.VMEM((CHUNKS * GROUP * PITCH, 128), jnp.float32),
            pltpu.VMEM((CHUNKS, GROUP, 32, 128), jnp.float32),
            pltpu.VMEM((CHUNKS, N, N), jnp.float32),
            pltpu.VMEM((CHUNKS * 128, 512), jnp.bfloat16),
            pltpu.VMEM((1024, 512), jnp.bfloat16),
            pltpu.VMEM((512, 512), jnp.bfloat16),
            pltpu.VMEM((N, 512), jnp.bfloat16),
            pltpu.VMEM((N, 512), jnp.bfloat16),
            pltpu.VMEM((512, N), jnp.bfloat16),
            pltpu.VMEM((512, N), jnp.bfloat16),
            pltpu.SemaphoreType.DMA((4, 4)),
            pltpu.SemaphoreType.DMA((4,)),
            pltpu.SemaphoreType.DMA((CHUNKS,)),
            pltpu.SemaphoreType.DMA((CHUNKS,)),
            pltpu.SemaphoreType.DMA((CHUNKS,)),
            pltpu.SemaphoreType.DMA((CHUNKS,)),
            pltpu.SemaphoreType.REGULAR((3,)),
        ],
        compiler_params=pltpu.CompilerParams(
            collective_id=0, has_side_effects=True, vmem_limit_bytes=50 * 1024 * 1024
        ),
    )(real_coeffs, imaginary_coeffs, np.concatenate([x_table(), z_table(), y_table()]))


def solution(mesh):
    placed = (P("sa", "px", "py", None), P("sa", "px", "py", None))
    return jax.shard_map(
        local,
        mesh=mesh,
        in_specs=placed,
        out_specs=P(None, ("px", "py"), "sa", None),
        check_vma=False,
    )
```

```python
import math

import jax
import jax.numpy as jnp
import numpy as np
from jax import lax
from jax.experimental import pallas as pl
from jax.experimental.pallas import tpu as pltpu
from jax.sharding import PartitionSpec as P

MESH = pl.DeviceIdType.MESH
corr_length = 1.0
log_spread = 0.5

N = 256
GROUP = 32
CHUNKS = 8
PITCH = 40


def matern(squared, length):
    return 1.0 / (1.0 + (2.0 * math.pi * corr_length / length) ** 2 * squared)


def matern_scale(length):
    middle = length // 2
    square_counts = {}
    for position in range(length):
        square_value = ((position + middle) % length - middle) ** 2
        square_counts[square_value] = square_counts.get(square_value, 0) + 1
    plane_counts = {}
    for first_square, first_count in square_counts.items():
        for second_square, second_count in square_counts.items():
            plane_sum = first_square + second_square
            plane_counts[plane_sum] = plane_counts.get(plane_sum, 0) + first_count * second_count
    running = 0.0
    for first_square, first_count in square_counts.items():
        for plane_sum, plane_count in plane_counts.items():
            running = (
                running + first_count * plane_count * matern(first_square + plane_sum, length) ** 2
            )
    return 1.0 / math.sqrt(running)


def halves(table):
    high = table.astype(np.float32).astype(jnp.bfloat16)
    low = (table - high.astype(np.float64)).astype(np.float32).astype(jnp.bfloat16)
    return high, low


def phases(rows, columns):
    angles = (np.asarray(rows)[:, None] * np.asarray(columns)[None, :] % N) * (2.0 * np.pi / N)
    return np.cos(angles), np.sin(angles)


def x_table():
    pieces = []
    for j in range(CHUNKS):
        cos, sin = phases(np.arange(GROUP) * CHUNKS + j, np.arange(N // 2))
        pieces += halves(np.block([[cos, -sin], [sin, cos]]))
    return np.concatenate(pieces, axis=0)


def z_table():
    owner, block, part, row = np.meshgrid(*(np.arange(n) for n in (8, 4, 2, 4)), indexing="ij")
    real = part.reshape(-1)[None, :] == 0
    pieces = []
    for odd in range(2):
        waves = (owner * 32 + (block * 4 + row) * 2 + odd).reshape(-1)
        cos, sin = phases(np.arange(N // 2), waves)
        pieces += halves(np.concatenate([np.where(real, cos, -sin), np.where(real, sin, cos)]))
    return np.concatenate(pieces, axis=0)


def y_table():
    cos, sin = phases(np.arange(N), np.arange(N))
    return np.concatenate([*halves(cos), *halves(-sin)], axis=0)


def split(value):
    high = value.astype(jnp.bfloat16)
    low = (value - high.astype(jnp.float32)).astype(jnp.bfloat16)
    return high, low


def dot(left, right, transposed):
    return lax.dot_general(
        left,
        right,
        (((1,), (1 if transposed else 0,)), ((), ())),
        preferred_element_type=jnp.float32,
    )


def signed(positions):
    return ((positions + N // 2) % N - N // 2).astype(jnp.float32)


def kernel(
    re_hbm, im_hbm, tables_hbm, out_ref,
    wbuf, xbuf, dhigh, dlow, gbuf, rbuf, obuf, tx, tz, ty, whigh, wlow, bhigh, blow,
    in_sem, table_sem, send_sem, recv_sem, out_send_sem, out_recv_sem, ready_sem,
):
    px, py, sa = lax.axis_index("px"), lax.axis_index("py"), lax.axis_index("sa")
    me = px * 8 + py
    z, y = px * 2 + lax.div(py, 4), lax.rem(py, 4)

    in_copies = []
    for block in range(4):
        group = []
        for part, source in enumerate((re_hbm, im_hbm)):
            for half in range(2):
                group.append(
                    pltpu.make_async_copy(
                        source.at[0, :, pl.ds(block * 8, 8), pl.ds(half * 128, 128)],
                        xbuf.at[part * 2 + half, :, pl.ds(block * 8, 8), :],
                        in_sem.at[block, part * 2 + half],
                    )
                )
        in_copies.append(group)
    table_copies = [
        pltpu.make_async_copy(
            tables_hbm.at[pl.ds(start, size), :], target.at[pl.ds(at, size), :], table_sem.at[i]
        )
        for i, (start, size, target, at) in enumerate(
            ((0, 128, tx, 0), (128, 896, tx, 128), (1024, 1024, tz, 0))
        )
    ] + [
        pltpu.make_async_copy(
            tables_hbm.at[pl.ds(2048 + part * 512, 512), :],
            ty.at[:, pl.ds(part * N, N)],
            table_sem.at[3 + part],
        )
        for part in range(2)
    ]
    for copy in in_copies[0]:
        copy.start()
    table_copies[0].start()

    def plane_peer(dz, dy):
        z2, y2 = lax.rem(z + (dz + 8) % 8, 8), lax.rem(y + dy, 4)
        return lax.div(z2, 2), lax.rem(z2, 2) * 4 + y2

    near, far = (
        [plane_peer(dz, dy) for dz in dzs for dy in range(4) if (dz, dy) != (0, 0)]
        for dzs in ((2, -2, 1, -1, 0), (4, 3, -3))
    )
    peers = far + near
    beside = [plane_peer(2, 0), plane_peer(-2, 0)]
    x, core = lax.div(sa, 2), lax.rem(sa, 2)
    others = [
        lax.rem(x + dx, 4) * 2 + lax.rem(core + dc, 2)
        for dx in (2, 1, 3, 0)
        for dc in range(2)
        if (dx, dc) != (0, 0)
    ]

    barrier = pltpu.get_barrier_semaphore()
    for p, q in near:
        pl.semaphore_signal(barrier, inc=1, device_id={"px": p, "py": q}, device_id_type=MESH)
    for other in others:
        pl.semaphore_signal(barrier, inc=1, device_id={"sa": other}, device_id_type=MESH)

    for group in in_copies[1:]:
        for copy in group:
            copy.start()
    for copy in table_copies[1:]:
        copy.start()

    scale = matern_scale(N)
    slope = (2.0 * math.pi * corr_length / N) ** 2
    fy = signed(lax.broadcasted_iota(jnp.int32, (64, 128), 0) + px * 64) ** 2
    lanes = lax.broadcasted_iota(jnp.int32, (64, 128), 1)
    flat = signed(lanes) ** 2 + fy, signed(lanes + 128) ** 2 + fy
    lines = xbuf.reshape(4, 64 * PITCH, 128)

    def prepare(k, carry):
        fz = signed(py * 32 + k) ** 2
        rows = pl.ds(pl.multiple_of(k * 64, 64), 64)
        for half in range(2):
            wbuf[half, rows, :] = (1.0 / (1.0 + slope * (flat[half] + fz))) * scale
        return carry

    def weigh(k, carry):
        rows = pl.ds(pl.multiple_of(k * 64, 64), 64)
        for part in range(2):
            columns = pl.ds(part * 128, 128)
            first, second = (
                lines[part * 2 + half, pl.ds(k, 64, stride=PITCH), :] * wbuf[half, rows, :]
                for half in range(2)
            )
            for odd, value in enumerate((first + second, first - second)):
                high, low = split(value)
                dhigh[odd, rows, columns] = high
                dlow[odd, rows, columns] = low
        return carry

    def transform(j, block):
        base = j * (GROUP * PITCH)
        table = pl.multiple_of(j * 128, 128)
        odd = j % 2 if isinstance(j, int) else lax.rem(j, 2)
        for piece in range(2):
            rows = pl.ds(block * 512 + piece * 256, 256)
            both = dot(tx[pl.ds(table, 128), :], dhigh[odd, rows, :], True)
            rest = dot(tx[pl.ds(table, 64), :], dlow[odd, rows, :], True)
            result = both[:64] + both[64:] + rest
            for part in range(2):
                for half in range(2):
                    at = base + block * 8 + part * 4 + piece * 2 + half
                    gbuf[pl.ds(at, GROUP, stride=PITCH), :] = result[
                        part * 32 : part * 32 + 32, half * 128 : half * 128 + 128
                    ]

    def send(targets, j, first, count):
        for p, q in targets:
            row = pl.multiple_of((j * GROUP + p * 8 + q) * PITCH + first, 8)
            pltpu.make_async_remote_copy(
                src_ref=gbuf.at[pl.ds(row, count), :],
                dst_ref=rbuf.at[j, me, pl.ds(first, count), :],
                send_sem=send_sem.at[j],
                recv_sem=recv_sem.at[j],
                device_id={"px": p, "py": q},
                device_id_type=MESH,
            ).start()

    def keep(j):
        rbuf[j, me] = gbuf[pl.ds(pl.multiple_of((j * GROUP + me) * PITCH, 8), 32), :]

    lax.fori_loop(0, 32, prepare, 0)
    for block in range(4):
        for copy in in_copies[block]:
            copy.wait()
        lax.fori_loop(block * 8, block * 8 + 8, weigh, 0)
        if block == 0:
            table_copies[0].wait()
        transform(0, block)
        if block == 1:
            pl.semaphore_wait(barrier, len(near) + len(others))
            for p, q in beside:
                pl.semaphore_signal(
                    ready_sem, inc=1, device_id={"px": p, "py": q}, device_id_type=MESH
                )
            send(near, 0, 0, 16)
    pl.semaphore_wait(ready_sem, len(beside))
    send(far, 0, 0, 32)
    send(near, 0, 16, 16)
    keep(0)
    table_copies[1].wait()

    def forward(j, carry):
        for block in range(4):
            transform(j, block)
        send(peers, j, 0, 32)
        keep(j)
        return carry

    lax.fori_loop(1, CHUNKS, forward, 0)
    for copy in table_copies[2:]:
        copy.wait()

    low_lanes = lax.broadcasted_iota(jnp.int32, (N, 128), 1) < 64

    def finish(j, carry):
        arrived = rbuf.at[j, pl.ds(0, GROUP - 1)]
        pltpu.make_async_copy(arrived, arrived, recv_sem.at[j]).wait()
        for pair in range(2):
            first, second = (
                rbuf[j, pl.ds((pair * 2 + k) * 8, 8)].reshape(N, 128) for k in range(2)
            )
            even = jnp.where(low_lanes, first, pltpu.roll(second, 64, 1))
            odd = jnp.where(low_lanes, pltpu.roll(first, 64, 1), second)
            for k, value in enumerate((even, odd)):
                rows = pl.ds(k * N, N)
                columns = pl.ds(pair * 128, 128)
                high, low = split(value)
                bhigh[rows, columns] = high
                blow[rows, columns] = low
        terms = []
        for odd in range(2):
            rows, above = pl.ds(odd * N, N), odd * 512
            both = dot(tz[above : above + 512], bhigh[rows, :], False)
            rest = dot(tz[above : above + N], blow[rows, :], False)
            terms.append(both[:N] + both[N:] + rest)
        for upper, value in enumerate((terms[0] + terms[1], terms[0] - terms[1])):
            rows = pl.ds(upper * 128, 128)
            for part in range(2):
                high, low = split(value[part * 128 : part * 128 + 128])
                whigh[rows, pl.ds(part * N, N)] = high
                wlow[rows, pl.ds(part * N, N)] = low
        both = dot(ty[...], whigh[...], True)
        field = both[:N] + both[N:] + dot(ty[:N], wlow[...], True)
        obuf[j] = jnp.exp(log_spread * field)
        for other in others:
            pltpu.make_async_remote_copy(
                src_ref=obuf.at[j, pl.ds(pl.multiple_of(other * 32, 32), 32), :],
                dst_ref=out_ref.at[sa, j],
                send_sem=out_send_sem.at[j],
                recv_sem=out_recv_sem.at[j],
                device_id={"sa": other},
                device_id_type=MESH,
            ).start()
        out_ref[sa, j] = obuf[j, pl.ds(pl.multiple_of(sa * 32, 32), 32), :]
        return carry

    lax.fori_loop(0, CHUNKS, finish, 0)

    def drain(j, carry):
        sent = rbuf.at[j, pl.ds(0, GROUP - 1)]
        pltpu.make_async_copy(sent, sent, send_sem.at[j]).wait()
        moved = obuf.at[j, pl.ds(0, 7 * 32), :]
        pltpu.make_async_copy(moved, moved, out_send_sem.at[j]).wait()
        pltpu.make_async_copy(moved, moved, out_recv_sem.at[j]).wait()
        return carry

    lax.fori_loop(0, CHUNKS, drain, 0)


def local(real_coeffs, imaginary_coeffs):
    anywhere = pl.BlockSpec(memory_space=pltpu.HBM)
    spare = np.zeros((2048, N), jnp.bfloat16)
    tables = np.concatenate([x_table(), z_table(), y_table(), spare])
    return pl.pallas_call(
        kernel,
        out_shape=jax.ShapeDtypeStruct((8, CHUNKS, 32, N), jnp.float32),
        in_specs=[anywhere] * 3,
        out_specs=pl.BlockSpec(memory_space=pltpu.VMEM),
        scratch_shapes=[
            pltpu.VMEM((2, 2048, 128), jnp.float32),
            pltpu.VMEM((4, 64, PITCH, 128), jnp.float32),
            pltpu.VMEM((2, 2048, N), jnp.bfloat16),
            pltpu.VMEM((2, 2048, N), jnp.bfloat16),
            pltpu.VMEM((CHUNKS * GROUP * PITCH, 128), jnp.float32),
            pltpu.VMEM((CHUNKS, GROUP, 32, 128), jnp.float32),
            pltpu.VMEM((CHUNKS, N, N), jnp.float32),
            pltpu.VMEM((CHUNKS * 128, N), jnp.bfloat16),
            pltpu.VMEM((1024, N), jnp.bfloat16),
            pltpu.VMEM((512, 512), jnp.bfloat16),
            pltpu.VMEM((N, 512), jnp.bfloat16),
            pltpu.VMEM((N, 512), jnp.bfloat16),
            pltpu.VMEM((512, N), jnp.bfloat16),
            pltpu.VMEM((512, N), jnp.bfloat16),
            pltpu.SemaphoreType.DMA((4, 4)),
            pltpu.SemaphoreType.DMA((5,)),
            pltpu.SemaphoreType.DMA((CHUNKS,)),
            pltpu.SemaphoreType.DMA((CHUNKS,)),
            pltpu.SemaphoreType.DMA((CHUNKS,)),
            pltpu.SemaphoreType.DMA((CHUNKS,)),
            pltpu.SemaphoreType.REGULAR,
        ],
        compiler_params=pltpu.CompilerParams(
            collective_id=0, has_side_effects=True, vmem_limit_bytes=50 * 1024 * 1024
        ),
    )(real_coeffs, imaginary_coeffs, tables)


def solution(mesh):
    placed = (P("sa", "px", "py", None), P("sa", "px", "py", None))
    return jax.shard_map(
        local,
        mesh=mesh,
        in_specs=placed,
        out_specs=P(None, ("px", "py"), "sa", None),
        check_vma=False,
    )
```

```python
import math

import jax
import jax.numpy as jnp
import numpy as np
from jax import lax
from jax.experimental import pallas as pl
from jax.experimental.pallas import tpu as pltpu
from jax.sharding import PartitionSpec as P

MESH = pl.DeviceIdType.MESH
corr_length = 1.0
log_spread = 0.5

N = 256
GROUP = 32
CHUNKS = 8
PITCH = 40


def matern(squared, length):
    return 1.0 / (1.0 + (2.0 * math.pi * corr_length / length) ** 2 * squared)


def matern_scale(length):
    middle = length // 2
    square_counts = {}
    for position in range(length):
        square_value = ((position + middle) % length - middle) ** 2
        square_counts[square_value] = square_counts.get(square_value, 0) + 1
    plane_counts = {}
    for first_square, first_count in square_counts.items():
        for second_square, second_count in square_counts.items():
            plane_sum = first_square + second_square
            plane_counts[plane_sum] = plane_counts.get(plane_sum, 0) + first_count * second_count
    running = 0.0
    for first_square, first_count in square_counts.items():
        for plane_sum, plane_count in plane_counts.items():
            running = (
                running + first_count * plane_count * matern(first_square + plane_sum, length) ** 2
            )
    return 1.0 / math.sqrt(running)


def halves(table):
    high = table.astype(np.float32).astype(jnp.bfloat16)
    low = (table - high.astype(np.float64)).astype(np.float32).astype(jnp.bfloat16)
    return high, low


def phases(rows, columns):
    angles = (np.asarray(rows)[:, None] * np.asarray(columns)[None, :] % N) * (2.0 * np.pi / N)
    return np.cos(angles), np.sin(angles)


def x_table():
    pieces = []
    for j in range(CHUNKS):
        cos, sin = phases(np.arange(GROUP) * CHUNKS + j, np.arange(N // 2))
        pieces += halves(np.block([[cos, -sin], [sin, cos]]))
    return np.concatenate(pieces, axis=0)


def z_table():
    owner, block, part, row = np.meshgrid(*(np.arange(n) for n in (8, 4, 2, 4)), indexing="ij")
    real = part.reshape(-1)[None, :] == 0
    pieces = []
    for odd in range(2):
        waves = (owner * 32 + (block * 4 + row) * 2 + odd).reshape(-1)
        cos, sin = phases(np.arange(N // 2), waves)
        pieces += halves(np.concatenate([np.where(real, cos, -sin), np.where(real, sin, cos)]))
    return np.concatenate(pieces, axis=0)


def y_table():
    cos, sin = phases(np.arange(N), np.arange(N))
    return np.concatenate([*halves(cos), *halves(-sin)], axis=0)


def split(value):
    high = value.astype(jnp.bfloat16)
    low = (value - high.astype(jnp.float32)).astype(jnp.bfloat16)
    return high, low


def dot(left, right, transposed):
    return lax.dot_general(
        left,
        right,
        (((1,), (1 if transposed else 0,)), ((), ())),
        preferred_element_type=jnp.float32,
    )


def signed(positions):
    return ((positions + N // 2) % N - N // 2).astype(jnp.float32)


def kernel(
    re_hbm, im_hbm, tables_hbm, out_ref,
    wbuf, xbuf, dhigh, dlow, gbuf, hbuf, rbuf, obuf, tx, tz, ty, whigh, wlow, bhigh, blow,
    in_sem, table_sem, send_sem, recv_sem, out_send_sem, out_recv_sem, mate_sem, ready_sem,
):
    px, py, sa = lax.axis_index("px"), lax.axis_index("py"), lax.axis_index("sa")
    me = px * 8 + py
    z, y = px * 2 + lax.div(py, 4), lax.rem(py, 4)

    in_copies = []
    for block in range(4):
        group = []
        for part, source in enumerate((re_hbm, im_hbm)):
            for half in range(2):
                group.append(
                    pltpu.make_async_copy(
                        source.at[0, :, pl.ds(block * 8, 8), pl.ds(half * 128, 128)],
                        xbuf.at[part * 2 + half, :, pl.ds(block * 8, 8), :],
                        in_sem.at[block, part * 2 + half],
                    )
                )
        in_copies.append(group)
    table_copies = [
        pltpu.make_async_copy(
            tables_hbm.at[pl.ds(start, size), :], target.at[pl.ds(at, size), :], table_sem.at[i]
        )
        for i, (start, size, target, at) in enumerate(
            ((0, 128, tx, 0), (128, 896, tx, 128), (1024, 1024, tz, 0))
        )
    ] + [
        pltpu.make_async_copy(
            tables_hbm.at[pl.ds(2048 + part * 512, 512), :],
            ty.at[:, pl.ds(part * N, N)],
            table_sem.at[3 + part],
        )
        for part in range(2)
    ]
    for copy in in_copies[0]:
        copy.start()
    table_copies[0].start()

    def plane_peer(dz, dy):
        z2, y2 = lax.rem(z + (dz + 8) % 8, 8), lax.rem(y + dy, 4)
        return lax.div(z2, 2), lax.rem(z2, 2) * 4 + y2

    near, far = (
        [plane_peer(dz, dy) for dz in dzs for dy in range(4) if (dz, dy) != (0, 0)]
        for dzs in ((2, -2, 1, -1, 0), (4, 3, -3))
    )
    peers = far + near
    beside = [plane_peer(2, 0), plane_peer(-2, 0)]
    x, core = lax.div(sa, 2), lax.rem(sa, 2)
    mate = x * 2 + (1 - core)
    places = [(dz, dy) for dz in (4, 3, -3, 2, -2, 1, -1, 0) for dy in (1, 0)]

    def shared(of_core):
        return [plane_peer(dz, of_core * 2 + dy) for dz, dy in places]

    others = [
        lax.rem(x + dx, 4) * 2 + lax.rem(core + dc, 2)
        for dx in (2, 1, 3, 0)
        for dc in range(2)
        if (dx, dc) != (0, 0)
    ]

    barrier = pltpu.get_barrier_semaphore()
    for p, q in near:
        pl.semaphore_signal(barrier, inc=1, device_id={"px": p, "py": q}, device_id_type=MESH)
    for other in others:
        pl.semaphore_signal(barrier, inc=1, device_id={"sa": other}, device_id_type=MESH)

    for group in in_copies[1:]:
        for copy in group:
            copy.start()
    for copy in table_copies[1:]:
        copy.start()

    scale = matern_scale(N)
    slope = (2.0 * math.pi * corr_length / N) ** 2
    fy = signed(lax.broadcasted_iota(jnp.int32, (64, 128), 0) + px * 64) ** 2
    lanes = lax.broadcasted_iota(jnp.int32, (64, 128), 1)
    flat = signed(lanes) ** 2 + fy, signed(lanes + 128) ** 2 + fy
    lines = xbuf.reshape(4, 64 * PITCH, 128)

    def prepare(k, carry):
        fz = signed(py * 32 + k) ** 2
        rows = pl.ds(pl.multiple_of(k * 64, 64), 64)
        for half in range(2):
            wbuf[half, rows, :] = (1.0 / (1.0 + slope * (flat[half] + fz))) * scale
        return carry

    def weigh(k, carry):
        rows = pl.ds(pl.multiple_of(k * 64, 64), 64)
        for part in range(2):
            columns = pl.ds(part * 128, 128)
            first, second = (
                lines[part * 2 + half, pl.ds(k, 64, stride=PITCH), :] * wbuf[half, rows, :]
                for half in range(2)
            )
            for odd, value in enumerate((first + second, first - second)):
                high, low = split(value)
                dhigh[odd, rows, columns] = high
                dlow[odd, rows, columns] = low
        return carry

    def transform(j, block):
        base = j * (GROUP * PITCH)
        table = pl.multiple_of(j * 128, 128)
        odd = j % 2 if isinstance(j, int) else lax.rem(j, 2)
        for piece in range(2):
            rows = pl.ds(block * 512 + piece * 256, 256)
            both = dot(tx[pl.ds(table, 128), :], dhigh[odd, rows, :], True)
            rest = dot(tx[pl.ds(table, 64), :], dlow[odd, rows, :], True)
            result = both[:64] + both[64:] + rest
            for part in range(2):
                for half in range(2):
                    at = base + block * 8 + part * 4 + piece * 2 + half
                    gbuf[pl.ds(at, GROUP, stride=PITCH), :] = result[
                        part * 32 : part * 32 + 32, half * 128 : half * 128 + 128
                    ]

    def send(targets, j, first, count):
        for p, q in targets:
            row = pl.multiple_of((j * GROUP + p * 8 + q) * PITCH + first, 8)
            pltpu.make_async_remote_copy(
                src_ref=gbuf.at[pl.ds(row, count), :],
                dst_ref=rbuf.at[j, me, pl.ds(first, count), :],
                send_sem=send_sem.at[j],
                recv_sem=recv_sem.at[j],
                device_id={"px": p, "py": q},
                device_id_type=MESH,
            ).start()

    def keep(j):
        rbuf[j, me] = gbuf[pl.ds(pl.multiple_of((j * GROUP + me) * PITCH, 8), 32), :]

    lax.fori_loop(0, 32, prepare, 0)
    for block in range(4):
        for copy in in_copies[block]:
            copy.wait()
        lax.fori_loop(block * 8, block * 8 + 8, weigh, 0)
        if block == 0:
            table_copies[0].wait()
        transform(0, block)
        if block == 1:
            pl.semaphore_wait(barrier, len(near) + len(others))
            for p, q in beside:
                pl.semaphore_signal(
                    ready_sem, inc=1, device_id={"px": p, "py": q}, device_id_type=MESH
                )
            send(near, 0, 0, 16)
    pl.semaphore_wait(ready_sem, len(beside))
    send(far, 0, 0, 32)
    send(near, 0, 16, 16)
    keep(0)
    table_copies[1].wait()

    last = CHUNKS - 1

    def message(p, q):
        return gbuf.at[pl.ds(pl.multiple_of((last * GROUP + p * 8 + q) * PITCH, 8), 32), :]

    for block in range(4):
        transform(last, block)
    keep(last)
    for slot, (p, q) in enumerate(shared(1 - core)):
        pltpu.make_async_remote_copy(
            src_ref=message(p, q),
            dst_ref=hbuf.at[slot],
            send_sem=mate_sem.at[0],
            recv_sem=mate_sem.at[1],
            device_id={"sa": mate},
            device_id_type=MESH,
        ).start()

    def forward(j, carry):
        for block in range(4):
            transform(j, block)
        send(peers, j, 0, 32)
        keep(j)
        return carry

    lax.fori_loop(1, last, forward, 0)
    pltpu.make_async_copy(hbuf, hbuf, mate_sem.at[1]).wait()

    def send_last(own):
        def one(slot, p, q):
            pltpu.make_async_remote_copy(
                src_ref=message(p, q) if own else hbuf.at[slot],
                dst_ref=rbuf.at[last, me],
                send_sem=send_sem.at[last],
                recv_sem=recv_sem.at[last],
                device_id={"px": p, "py": q, "sa": sa if own else mate},
                device_id_type=MESH,
            ).start()

        *most, final = shared(core)
        for slot, (p, q) in enumerate(most):
            one(slot, p, q)
        pl.when(core == 1)(lambda: one(len(most), *final))

    @pl.when(core == 0)
    def _():
        send_last(True)
        send_last(False)

    @pl.when(core == 1)
    def _():
        send_last(False)
        send_last(True)

    for copy in table_copies[2:]:
        copy.wait()

    low_lanes = lax.broadcasted_iota(jnp.int32, (N, 128), 1) < 64

    def finish(j, carry):
        arrived = rbuf.at[j, pl.ds(0, GROUP - 1)]
        pltpu.make_async_copy(arrived, arrived, recv_sem.at[j]).wait()
        for pair in range(2):
            first, second = (
                rbuf[j, pl.ds((pair * 2 + k) * 8, 8)].reshape(N, 128) for k in range(2)
            )
            even = jnp.where(low_lanes, first, pltpu.roll(second, 64, 1))
            odd = jnp.where(low_lanes, pltpu.roll(first, 64, 1), second)
            for k, value in enumerate((even, odd)):
                rows = pl.ds(k * N, N)
                columns = pl.ds(pair * 128, 128)
                high, low = split(value)
                bhigh[rows, columns] = high
                blow[rows, columns] = low
        terms = []
        for odd in range(2):
            rows, above = pl.ds(odd * N, N), odd * 512
            both = dot(tz[above : above + 512], bhigh[rows, :], False)
            rest = dot(tz[above : above + N], blow[rows, :], False)
            terms.append(both[:N] + both[N:] + rest)
        for upper, value in enumerate((terms[0] + terms[1], terms[0] - terms[1])):
            rows = pl.ds(upper * 128, 128)
            for part in range(2):
                high, low = split(value[part * 128 : part * 128 + 128])
                whigh[rows, pl.ds(part * N, N)] = high
                wlow[rows, pl.ds(part * N, N)] = low
        both = dot(ty[...], whigh[...], True)
        field = both[:N] + both[N:] + dot(ty[:N], wlow[...], True)
        obuf[j] = jnp.exp(log_spread * field)
        for other in others:
            pltpu.make_async_remote_copy(
                src_ref=obuf.at[j, pl.ds(pl.multiple_of(other * 32, 32), 32), :],
                dst_ref=out_ref.at[sa, j],
                send_sem=out_send_sem.at[j],
                recv_sem=out_recv_sem.at[j],
                device_id={"sa": other},
                device_id_type=MESH,
            ).start()
        out_ref[sa, j] = obuf[j, pl.ds(pl.multiple_of(sa * 32, 32), 32), :]
        return carry

    lax.fori_loop(0, CHUNKS, finish, 0)

    for served in range(2):
        sent = rbuf.at[last, pl.ds(0, 30 + 2 * served)]
        pl.when(core == served)(pltpu.make_async_copy(sent, sent, send_sem.at[last]).wait)
    pltpu.make_async_copy(hbuf, hbuf, mate_sem.at[0]).wait()

    def drain_sent(j, carry):
        sent = rbuf.at[j, pl.ds(0, GROUP - 1)]
        pltpu.make_async_copy(sent, sent, send_sem.at[j]).wait()
        return carry

    lax.fori_loop(0, last, drain_sent, 0)

    def drain(j, carry):
        moved = obuf.at[j, pl.ds(0, 7 * 32), :]
        pltpu.make_async_copy(moved, moved, out_send_sem.at[j]).wait()
        pltpu.make_async_copy(moved, moved, out_recv_sem.at[j]).wait()
        return carry

    lax.fori_loop(0, CHUNKS, drain, 0)


def local(real_coeffs, imaginary_coeffs):
    anywhere = pl.BlockSpec(memory_space=pltpu.HBM)
    spare = np.zeros((2048, N), jnp.bfloat16)
    tables = np.concatenate([x_table(), z_table(), y_table(), spare])
    return pl.pallas_call(
        kernel,
        out_shape=jax.ShapeDtypeStruct((8, CHUNKS, 32, N), jnp.float32),
        in_specs=[anywhere] * 3,
        out_specs=pl.BlockSpec(memory_space=pltpu.VMEM),
        scratch_shapes=[
            pltpu.VMEM((2, 2048, 128), jnp.float32),
            pltpu.VMEM((4, 64, PITCH, 128), jnp.float32),
            pltpu.VMEM((2, 2048, N), jnp.bfloat16),
            pltpu.VMEM((2, 2048, N), jnp.bfloat16),
            pltpu.VMEM((CHUNKS * GROUP * PITCH, 128), jnp.float32),
            pltpu.VMEM((GROUP // 2, 32, 128), jnp.float32),
            pltpu.VMEM((CHUNKS, GROUP, 32, 128), jnp.float32),
            pltpu.VMEM((CHUNKS, N, N), jnp.float32),
            pltpu.VMEM((CHUNKS * 128, N), jnp.bfloat16),
            pltpu.VMEM((1024, N), jnp.bfloat16),
            pltpu.VMEM((512, 512), jnp.bfloat16),
            pltpu.VMEM((N, 512), jnp.bfloat16),
            pltpu.VMEM((N, 512), jnp.bfloat16),
            pltpu.VMEM((512, N), jnp.bfloat16),
            pltpu.VMEM((512, N), jnp.bfloat16),
            pltpu.SemaphoreType.DMA((4, 4)),
            pltpu.SemaphoreType.DMA((5,)),
            pltpu.SemaphoreType.DMA((CHUNKS,)),
            pltpu.SemaphoreType.DMA((CHUNKS,)),
            pltpu.SemaphoreType.DMA((CHUNKS,)),
            pltpu.SemaphoreType.DMA((CHUNKS,)),
            pltpu.SemaphoreType.DMA((2,)),
            pltpu.SemaphoreType.REGULAR,
        ],
        compiler_params=pltpu.CompilerParams(
            collective_id=0, has_side_effects=True, vmem_limit_bytes=50 * 1024 * 1024
        ),
    )(real_coeffs, imaginary_coeffs, tables)


def solution(mesh):
    placed = (P("sa", "px", "py", None), P("sa", "px", "py", None))
    return jax.shard_map(
        local,
        mesh=mesh,
        in_specs=placed,
        out_specs=P(None, ("px", "py"), "sa", None),
        check_vma=False,
    )
```

```python
import math

import jax
import jax.numpy as jnp
import numpy as np
from jax import lax
from jax.experimental import pallas as pl
from jax.experimental.pallas import tpu as pltpu
from jax.sharding import PartitionSpec as P

MESH = pl.DeviceIdType.MESH
corr_length = 1.0
log_spread = 0.5

N = 256
GROUP = 32
CHUNKS = 8
PITCH = 40


def matern(squared, length):
    return 1.0 / (1.0 + (2.0 * math.pi * corr_length / length) ** 2 * squared)


def matern_scale(length):
    middle = length // 2
    square_counts = {}
    for position in range(length):
        square_value = ((position + middle) % length - middle) ** 2
        square_counts[square_value] = square_counts.get(square_value, 0) + 1
    plane_counts = {}
    for first_square, first_count in square_counts.items():
        for second_square, second_count in square_counts.items():
            plane_sum = first_square + second_square
            plane_counts[plane_sum] = plane_counts.get(plane_sum, 0) + first_count * second_count
    running = 0.0
    for first_square, first_count in square_counts.items():
        for plane_sum, plane_count in plane_counts.items():
            running = (
                running + first_count * plane_count * matern(first_square + plane_sum, length) ** 2
            )
    return 1.0 / math.sqrt(running)


def halves(table):
    high = table.astype(np.float32).astype(jnp.bfloat16)
    low = (table - high.astype(np.float64)).astype(np.float32).astype(jnp.bfloat16)
    return high, low


def phases(rows, columns):
    angles = (np.asarray(rows)[:, None] * np.asarray(columns)[None, :] % N) * (2.0 * np.pi / N)
    return np.cos(angles), np.sin(angles)


def x_table():
    pieces = []
    for j in range(CHUNKS):
        cos, sin = phases(np.arange(GROUP) * CHUNKS + j, np.arange(N // 2))
        pieces += halves(np.block([[cos, -sin], [sin, cos]]))
    return np.concatenate(pieces, axis=0)


def z_table():
    owner, block, part, row = np.meshgrid(*(np.arange(n) for n in (8, 4, 2, 4)), indexing="ij")
    real = part.reshape(-1)[None, :] == 0
    pieces = []
    for odd in range(2):
        waves = (owner * 32 + (block * 4 + row) * 2 + odd).reshape(-1)
        cos, sin = phases(np.arange(N // 2), waves)
        pieces += halves(np.concatenate([np.where(real, cos, -sin), np.where(real, sin, cos)]))
    return np.concatenate(pieces, axis=0)


def y_table():
    cos, sin = phases(np.arange(N), np.arange(N))
    return np.concatenate([*halves(cos), *halves(-sin)], axis=0)


def split(value):
    high = value.astype(jnp.bfloat16)
    low = (value - high.astype(jnp.float32)).astype(jnp.bfloat16)
    return high, low


def dot(left, right, transposed):
    return lax.dot_general(
        left,
        right,
        (((1,), (1 if transposed else 0,)), ((), ())),
        preferred_element_type=jnp.float32,
    )


def signed(positions):
    return ((positions + N // 2) % N - N // 2).astype(jnp.float32)


def kernel(
    re_hbm, im_hbm, tables_hbm, out_ref,
    wbuf, xbuf, dhigh, dlow, gbuf, hbuf, rbuf, obuf, tx, tz, ty, whigh, wlow, bhigh, blow,
    in_sem, table_sem, send_sem, recv_sem, out_send_sem, out_recv_sem, mate_sem, ready_sem,
):
    px, py, sa = lax.axis_index("px"), lax.axis_index("py"), lax.axis_index("sa")
    me = px * 8 + py
    z, y = px * 2 + lax.div(py, 4), lax.rem(py, 4)

    in_copies = []
    for block in range(4):
        group = []
        for part, source in enumerate((re_hbm, im_hbm)):
            for half in range(2):
                group.append(
                    pltpu.make_async_copy(
                        source.at[0, :, pl.ds(block * 8, 8), pl.ds(half * 128, 128)],
                        xbuf.at[part * 2 + half, :, pl.ds(block * 8, 8), :],
                        in_sem.at[block, part * 2 + half],
                    )
                )
        in_copies.append(group)
    table_copies = [
        pltpu.make_async_copy(
            tables_hbm.at[pl.ds(start, size), :], target.at[pl.ds(at, size), :], table_sem.at[i]
        )
        for i, (start, size, target, at) in enumerate(
            ((0, 128, tx, 0), (128, 896, tx, 128), (1024, 1024, tz, 0))
        )
    ]
    for copy in in_copies[0]:
        copy.start()
    table_copies[0].start()

    def plane_peer(dz, dy):
        z2, y2 = lax.rem(z + (dz + 8) % 8, 8), lax.rem(y + dy, 4)
        return lax.div(z2, 2), lax.rem(z2, 2) * 4 + y2

    near, far = (
        [plane_peer(dz, dy) for dz in dzs for dy in range(4) if (dz, dy) != (0, 0)]
        for dzs in ((2, -2, 1, -1, 0), (4, 3, -3))
    )
    peers = far + near
    beside = [plane_peer(2, 0), plane_peer(-2, 0)]
    x, core = lax.div(sa, 2), lax.rem(sa, 2)
    mate = x * 2 + (1 - core)
    places = [(dz, dy) for dz in (4, 3, -3, 2, -2, 1, -1, 0) for dy in (1, 0)]

    def shared(of_core):
        return [plane_peer(dz, of_core * 2 + dy) for dz, dy in places]

    others = [
        lax.rem(x + dx, 4) * 2 + lax.rem(core + dc, 2)
        for dx, dc in ((2, 1), (2, 0), (1, 1), (3, 1), (1, 0), (3, 0), (0, 1))
    ]

    barrier = pltpu.get_barrier_semaphore()
    for p, q in near:
        pl.semaphore_signal(barrier, inc=1, device_id={"px": p, "py": q}, device_id_type=MESH)
    for other in others:
        pl.semaphore_signal(barrier, inc=1, device_id={"sa": other}, device_id_type=MESH)

    for group in in_copies[1:]:
        for copy in group:
            copy.start()
    for copy in table_copies[1:]:
        copy.start()
    scale = matern_scale(N)
    slope = (2.0 * math.pi * corr_length / N) ** 2
    fy = signed(lax.broadcasted_iota(jnp.int32, (64, 128), 0) + px * 64) ** 2
    lanes = lax.broadcasted_iota(jnp.int32, (64, 128), 1)
    flat = signed(lanes) ** 2 + fy, signed(lanes + 128) ** 2 + fy
    lines = xbuf.reshape(4, 64 * PITCH, 128)

    def prepare(k, carry):
        fz = signed(py * 32 + k) ** 2
        rows = pl.ds(pl.multiple_of(k * 64, 64), 64)
        for half in range(2):
            wbuf[half, rows, :] = (1.0 / (1.0 + slope * (flat[half] + fz))) * scale
        return carry

    def weigh(k, carry):
        rows = pl.ds(pl.multiple_of(k * 64, 64), 64)
        for part in range(2):
            columns = pl.ds(part * 128, 128)
            first, second = (
                lines[part * 2 + half, pl.ds(k, 64, stride=PITCH), :] * wbuf[half, rows, :]
                for half in range(2)
            )
            for odd, value in enumerate((first + second, first - second)):
                high, low = split(value)
                dhigh[odd, rows, columns] = high
                dlow[odd, rows, columns] = low
        return carry

    def transform(j, block):
        base = j * (GROUP * PITCH)
        table = pl.multiple_of(j * 128, 128)
        odd = j % 2 if isinstance(j, int) else lax.rem(j, 2)
        for piece in range(2):
            rows = pl.ds(block * 512 + piece * 256, 256)
            both = dot(tx[pl.ds(table, 128), :], dhigh[odd, rows, :], True)
            rest = dot(tx[pl.ds(table, 64), :], dlow[odd, rows, :], True)
            result = both[:64] + both[64:] + rest
            for part in range(2):
                for half in range(2):
                    at = base + block * 8 + part * 4 + piece * 2 + half
                    gbuf[pl.ds(at, GROUP, stride=PITCH), :] = result[
                        part * 32 : part * 32 + 32, half * 128 : half * 128 + 128
                    ]

    def send(targets, j, first, count):
        for p, q in targets:
            row = pl.multiple_of((j * GROUP + p * 8 + q) * PITCH + first, 8)
            pltpu.make_async_remote_copy(
                src_ref=gbuf.at[pl.ds(row, count), :],
                dst_ref=rbuf.at[j, me, pl.ds(first, count), :],
                send_sem=send_sem.at[j],
                recv_sem=recv_sem.at[j],
                device_id={"px": p, "py": q},
                device_id_type=MESH,
            ).start()

    def keep(j):
        rbuf[j, me] = gbuf[pl.ds(pl.multiple_of((j * GROUP + me) * PITCH, 8), 32), :]

    lax.fori_loop(0, 32, prepare, 0)
    for block in range(4):
        for copy in in_copies[block]:
            copy.wait()
        lax.fori_loop(block * 8, block * 8 + 8, weigh, 0)
        if block == 0:
            table_copies[0].wait()
        transform(0, block)
        if block == 0:
            pl.semaphore_wait(barrier, len(near) + len(others))
            for p, q in beside:
                pl.semaphore_signal(
                    ready_sem, inc=1, device_id={"px": p, "py": q}, device_id_type=MESH
                )
        if block < 3:
            send(near, 0, block * 8, 8)
    pl.semaphore_wait(ready_sem, len(beside))
    send(far, 0, 0, 32)
    send(near, 0, 24, 8)
    keep(0)

    for part in range(2):
        for precision in range(2):
            for place, owner in enumerate([*others, sa]):
                half, slot = divmod(place, 4)
                pltpu.make_async_copy(
                    tables_hbm.at[
                        pl.ds(pl.multiple_of(2048 + part * 512 + precision * N + owner * 32, 32), 32), :
                    ],
                    ty.at[pl.ds(half * N + precision * 128 + slot * 32, 32), pl.ds(part * N, N)],
                    table_sem.at[3],
                ).start()

    table_copies[1].wait()

    last = CHUNKS - 1

    def message(p, q):
        return gbuf.at[pl.ds(pl.multiple_of((last * GROUP + p * 8 + q) * PITCH, 8), 32), :]

    for block in range(4):
        transform(last, block)
    keep(last)
    for slot, (p, q) in enumerate(shared(1 - core)):
        pltpu.make_async_remote_copy(
            src_ref=message(p, q),
            dst_ref=hbuf.at[slot],
            send_sem=mate_sem.at[0],
            recv_sem=mate_sem.at[1],
            device_id={"sa": mate},
            device_id_type=MESH,
        ).start()

    def forward(j, carry):
        for block in range(4):
            transform(j, block)
        send(peers, j, 0, 32)
        keep(j)
        return carry

    lax.fori_loop(1, last, forward, 0)
    pltpu.make_async_copy(hbuf, hbuf, mate_sem.at[1]).wait()

    def send_last(own):
        def one(slot, p, q):
            pltpu.make_async_remote_copy(
                src_ref=message(p, q) if own else hbuf.at[slot],
                dst_ref=rbuf.at[last, me],
                send_sem=send_sem.at[last],
                recv_sem=recv_sem.at[last],
                device_id={"px": p, "py": q, "sa": sa if own else mate},
                device_id_type=MESH,
            ).start()

        *most, final = shared(core)
        for slot, (p, q) in enumerate(most):
            one(slot, p, q)
        pl.when(core == 1)(lambda: one(len(most), *final))

    @pl.when(core == 0)
    def _():
        send_last(True)
        send_last(False)

    @pl.when(core == 1)
    def _():
        send_last(False)
        send_last(True)

    table_copies[2].wait()
    pltpu.make_async_copy(ty, ty, table_sem.at[3]).wait()

    low_lanes = lax.broadcasted_iota(jnp.int32, (N, 128), 1) < 64

    def finish(j, carry):
        arrived = rbuf.at[j, pl.ds(0, GROUP - 1)]
        pltpu.make_async_copy(arrived, arrived, recv_sem.at[j]).wait()
        for pair in range(2):
            first, second = (
                rbuf[j, pl.ds((pair * 2 + k) * 8, 8)].reshape(N, 128) for k in range(2)
            )
            even = jnp.where(low_lanes, first, pltpu.roll(second, 64, 1))
            odd = jnp.where(low_lanes, pltpu.roll(first, 64, 1), second)
            for k, value in enumerate((even, odd)):
                rows = pl.ds(k * N, N)
                columns = pl.ds(pair * 128, 128)
                high, low = split(value)
                bhigh[rows, columns] = high
                blow[rows, columns] = low
        terms = []
        for odd in range(2):
            rows, above = pl.ds(odd * N, N), odd * 512
            high, low = tz[above : above + N], tz[above + N : above + 2 * N]
            terms.append(
                dot(high, bhigh[rows, :], False)
                + dot(low, bhigh[rows, :], False)
                + dot(high, blow[rows, :], False)
            )
        for upper, value in enumerate((terms[0] + terms[1], terms[0] - terms[1])):
            rows = pl.ds(upper * 128, 128)
            for part in range(2):
                high, low = split(value[part * 128 : part * 128 + 128])
                whigh[rows, pl.ds(part * N, N)] = high
                wlow[rows, pl.ds(part * N, N)] = low
        for half in range(2):
            both = dot(ty[half * N : half * N + N], whigh[...], True)
            field = both[:128] + both[128:] + dot(ty[half * N : half * N + 128], wlow[...], True)
            obuf[j, pl.ds(half * 128, 128), :] = jnp.exp(log_spread * field)
            for place, other in enumerate(others):
                if place // 4 != half:
                    continue
                pltpu.make_async_remote_copy(
                    src_ref=obuf.at[j, pl.ds(place * 32, 32), :],
                    dst_ref=out_ref.at[sa, j],
                    send_sem=out_send_sem.at[j],
                    recv_sem=out_recv_sem.at[j],
                    device_id={"sa": other},
                    device_id_type=MESH,
                ).start()
        out_ref[sa, j] = obuf[j, pl.ds(7 * 32, 32), :]
        return carry

    lax.fori_loop(0, CHUNKS, finish, 0)

    for served in range(2):
        sent = rbuf.at[last, pl.ds(0, 30 + 2 * served)]
        pl.when(core == served)(pltpu.make_async_copy(sent, sent, send_sem.at[last]).wait)
    pltpu.make_async_copy(hbuf, hbuf, mate_sem.at[0]).wait()

    def drain_sent(j, carry):
        sent = rbuf.at[j, pl.ds(0, GROUP - 1)]
        pltpu.make_async_copy(sent, sent, send_sem.at[j]).wait()
        return carry

    lax.fori_loop(0, last, drain_sent, 0)

    def drain(j, carry):
        moved = obuf.at[j, pl.ds(0, 7 * 32), :]
        pltpu.make_async_copy(moved, moved, out_send_sem.at[j]).wait()
        pltpu.make_async_copy(moved, moved, out_recv_sem.at[j]).wait()
        return carry

    lax.fori_loop(0, CHUNKS, drain, 0)


def local(real_coeffs, imaginary_coeffs):
    anywhere = pl.BlockSpec(memory_space=pltpu.HBM)
    spare = np.zeros((2048, N), jnp.bfloat16)
    tables = np.concatenate([x_table(), z_table(), y_table(), spare])
    return pl.pallas_call(
        kernel,
        out_shape=jax.ShapeDtypeStruct((8, CHUNKS, 32, N), jnp.float32),
        in_specs=[anywhere] * 3,
        out_specs=pl.BlockSpec(memory_space=pltpu.VMEM),
        scratch_shapes=[
            pltpu.VMEM((2, 2048, 128), jnp.float32),
            pltpu.VMEM((4, 64, PITCH, 128), jnp.float32),
            pltpu.VMEM((2, 2048, N), jnp.bfloat16),
            pltpu.VMEM((2, 2048, N), jnp.bfloat16),
            pltpu.VMEM((CHUNKS * GROUP * PITCH, 128), jnp.float32),
            pltpu.VMEM((GROUP // 2, 32, 128), jnp.float32),
            pltpu.VMEM((CHUNKS, GROUP, 32, 128), jnp.float32),
            pltpu.VMEM((CHUNKS, N, N), jnp.float32),
            pltpu.VMEM((CHUNKS * 128, N), jnp.bfloat16),
            pltpu.VMEM((1024, N), jnp.bfloat16),
            pltpu.VMEM((512, 512), jnp.bfloat16),
            pltpu.VMEM((N, 512), jnp.bfloat16),
            pltpu.VMEM((N, 512), jnp.bfloat16),
            pltpu.VMEM((512, N), jnp.bfloat16),
            pltpu.VMEM((512, N), jnp.bfloat16),
            pltpu.SemaphoreType.DMA((4, 4)),
            pltpu.SemaphoreType.DMA((4,)),
            pltpu.SemaphoreType.DMA((CHUNKS,)),
            pltpu.SemaphoreType.DMA((CHUNKS,)),
            pltpu.SemaphoreType.DMA((CHUNKS,)),
            pltpu.SemaphoreType.DMA((CHUNKS,)),
            pltpu.SemaphoreType.DMA((2,)),
            pltpu.SemaphoreType.REGULAR,
        ],
        compiler_params=pltpu.CompilerParams(
            collective_id=0, has_side_effects=True, vmem_limit_bytes=50 * 1024 * 1024
        ),
    )(real_coeffs, imaginary_coeffs, tables)


def solution(mesh):
    placed = (P("sa", "px", "py", None), P("sa", "px", "py", None))
    return jax.shard_map(
        local,
        mesh=mesh,
        in_specs=placed,
        out_specs=P(None, ("px", "py"), "sa", None),
        check_vma=False,
    )
```

```python
import math

import jax
import jax.numpy as jnp
import numpy as np
from jax import lax
from jax.experimental import pallas as pl
from jax.experimental.pallas import tpu as pltpu
from jax.sharding import PartitionSpec as P

MESH = pl.DeviceIdType.MESH
corr_length = 1.0
log_spread = 0.5

N = 256
GROUP = 32
CHUNKS = 8
PITCH = 40


def matern(squared, length):
    return 1.0 / (1.0 + (2.0 * math.pi * corr_length / length) ** 2 * squared)


def matern_scale(length):
    middle = length // 2
    square_counts = {}
    for position in range(length):
        square_value = ((position + middle) % length - middle) ** 2
        square_counts[square_value] = square_counts.get(square_value, 0) + 1
    plane_counts = {}
    for first_square, first_count in square_counts.items():
        for second_square, second_count in square_counts.items():
            plane_sum = first_square + second_square
            plane_counts[plane_sum] = plane_counts.get(plane_sum, 0) + first_count * second_count
    running = 0.0
    for first_square, first_count in square_counts.items():
        for plane_sum, plane_count in plane_counts.items():
            running = (
                running + first_count * plane_count * matern(first_square + plane_sum, length) ** 2
            )
    return 1.0 / math.sqrt(running)


def halves(table):
    high = table.astype(np.float32).astype(jnp.bfloat16)
    low = (table - high.astype(np.float64)).astype(np.float32).astype(jnp.bfloat16)
    return high, low


def phases(rows, columns):
    angles = (np.asarray(rows)[:, None] * np.asarray(columns)[None, :] % N) * (2.0 * np.pi / N)
    return np.cos(angles), np.sin(angles)


def x_table():
    pieces = []
    for j in range(CHUNKS):
        cos, sin = phases(np.arange(GROUP) * CHUNKS + j, np.arange(N // 2))
        pieces += halves(np.block([[cos, -sin], [sin, cos]]))
    return np.concatenate(pieces, axis=0)


def z_table():
    owner, block, part, row = np.meshgrid(*(np.arange(n) for n in (8, 4, 2, 4)), indexing="ij")
    real = part.reshape(-1)[None, :] == 0
    pieces = []
    for odd in range(2):
        waves = (owner * 32 + (block * 4 + row) * 2 + odd).reshape(-1)
        cos, sin = phases(np.arange(N // 2), waves)
        pieces += halves(np.concatenate([np.where(real, cos, -sin), np.where(real, sin, cos)]))
    return np.concatenate(pieces, axis=0)


def y_table():
    cos, sin = phases(np.arange(N), np.arange(N))
    return np.concatenate([*halves(cos), *halves(-sin)], axis=0)


def split(value):
    high = value.astype(jnp.bfloat16)
    low = (value - high.astype(jnp.float32)).astype(jnp.bfloat16)
    return high, low


def dot(left, right, transposed):
    return lax.dot_general(
        left,
        right,
        (((1,), (1 if transposed else 0,)), ((), ())),
        preferred_element_type=jnp.float32,
    )


def signed(positions):
    return ((positions + N // 2) % N - N // 2).astype(jnp.float32)


def kernel(
    re_hbm, im_hbm, tables_hbm, out_ref,
    wbuf, xbuf, dhigh, dlow, gbuf, hbuf, rbuf, obuf, tx, tz, ty, whigh, wlow, bhigh, blow,
    in_sem, table_sem, send_sem, recv_sem, out_send_sem, out_recv_sem, mate_sem, ready_sem,
):
    px, py, sa = lax.axis_index("px"), lax.axis_index("py"), lax.axis_index("sa")
    me = px * 8 + py
    z, y = px * 2 + lax.div(py, 4), lax.rem(py, 4)

    in_copies = []
    for block in range(4):
        group = []
        for part, source in enumerate((re_hbm, im_hbm)):
            for half in range(2):
                group.append(
                    pltpu.make_async_copy(
                        source.at[0, :, pl.ds(block * 8, 8), pl.ds(half * 128, 128)],
                        xbuf.at[part * 2 + half, :, pl.ds(block * 8, 8), :],
                        in_sem.at[block, part * 2 + half],
                    )
                )
        in_copies.append(group)
    table_copies = [
        pltpu.make_async_copy(
            tables_hbm.at[pl.ds(start, size), :], target.at[pl.ds(at, size), :], table_sem.at[i]
        )
        for i, (start, size, target, at) in enumerate(
            ((0, 128, tx, 0), (128, 896, tx, 128), (1024, 1024, tz, 0))
        )
    ]
    for copy in in_copies[0]:
        copy.start()
    table_copies[0].start()

    def plane_peer(dz, dy):
        z2, y2 = lax.rem(z + (dz + 8) % 8, 8), lax.rem(y + dy, 4)
        return lax.div(z2, 2), lax.rem(z2, 2) * 4 + y2

    near, far = (
        [plane_peer(dz, dy) for dz in dzs for dy in range(4) if (dz, dy) != (0, 0)]
        for dzs in ((2, -2, 1, -1, 0), (4, 3, -3))
    )
    peers = far + near
    beside = [plane_peer(2, 0), plane_peer(-2, 0)]
    x, core = lax.div(sa, 2), lax.rem(sa, 2)
    mate = x * 2 + (1 - core)
    places = [(dz, dy) for dz in (4, 3, -3, 2, -2, 1, -1, 0) for dy in (1, 0)]

    def shared(of_core):
        return [plane_peer(dz, of_core * 2 + dy) for dz, dy in places]

    others = [
        lax.rem(x + dx, 4) * 2 + lax.rem(core + dc, 2)
        for dx, dc in ((2, 0), (2, 1), (1, 0), (3, 0), (1, 1), (3, 1), (0, 1))
    ]

    barrier = pltpu.get_barrier_semaphore()
    for p, q in near:
        pl.semaphore_signal(barrier, inc=1, device_id={"px": p, "py": q}, device_id_type=MESH)
    for other in others:
        pl.semaphore_signal(barrier, inc=1, device_id={"sa": other}, device_id_type=MESH)

    for group in in_copies[1:]:
        for copy in group:
            copy.start()
    for copy in table_copies[1:]:
        copy.start()
    for part in range(2):
        for precision in range(2):
            for place, owner in enumerate([*others, sa]):
                half, slot = divmod(place, 4)
                pltpu.make_async_copy(
                    tables_hbm.at[
                        pl.ds(pl.multiple_of(2048 + part * 512 + precision * N + owner * 32, 32), 32), :
                    ],
                    ty.at[pl.ds(half * N + precision * 128 + slot * 32, 32), pl.ds(part * N, N)],
                    table_sem.at[3],
                ).start()

    scale = matern_scale(N)
    slope = (2.0 * math.pi * corr_length / N) ** 2
    fy = signed(lax.broadcasted_iota(jnp.int32, (64, 128), 0) + px * 64) ** 2
    lanes = lax.broadcasted_iota(jnp.int32, (64, 128), 1)
    flat = signed(lanes) ** 2 + fy, signed(lanes + 128) ** 2 + fy
    lines = xbuf.reshape(4, 64 * PITCH, 128)

    def prepare(k, carry):
        fz = signed(py * 32 + k) ** 2
        rows = pl.ds(pl.multiple_of(k * 64, 64), 64)
        for half in range(2):
            wbuf[half, rows, :] = (1.0 / (1.0 + slope * (flat[half] + fz))) * scale
        return carry

    def weigh(k, carry):
        rows = pl.ds(pl.multiple_of(k * 64, 64), 64)
        for part in range(2):
            columns = pl.ds(part * 128, 128)
            first, second = (
                lines[part * 2 + half, pl.ds(k, 64, stride=PITCH), :] * wbuf[half, rows, :]
                for half in range(2)
            )
            for odd, value in enumerate((first + second, first - second)):
                high, low = split(value)
                dhigh[odd, rows, columns] = high
                dlow[odd, rows, columns] = low
        return carry

    def transform(j, block):
        base = j * (GROUP * PITCH)
        table = pl.multiple_of(j * 128, 128)
        odd = j % 2 if isinstance(j, int) else lax.rem(j, 2)
        for piece in range(2):
            rows = pl.ds(block * 512 + piece * 256, 256)
            both = dot(tx[pl.ds(table, 128), :], dhigh[odd, rows, :], True)
            rest = dot(tx[pl.ds(table, 64), :], dlow[odd, rows, :], True)
            result = both[:64] + both[64:] + rest
            for part in range(2):
                for half in range(2):
                    at = base + block * 8 + part * 4 + piece * 2 + half
                    gbuf[pl.ds(at, GROUP, stride=PITCH), :] = result[
                        part * 32 : part * 32 + 32, half * 128 : half * 128 + 128
                    ]

    def send(targets, j, first, count):
        for p, q in targets:
            row = pl.multiple_of((j * GROUP + p * 8 + q) * PITCH + first, 8)
            pltpu.make_async_remote_copy(
                src_ref=gbuf.at[pl.ds(row, count), :],
                dst_ref=rbuf.at[j, me, pl.ds(first, count), :],
                send_sem=send_sem.at[j],
                recv_sem=recv_sem.at[j],
                device_id={"px": p, "py": q},
                device_id_type=MESH,
            ).start()

    def keep(j):
        rbuf[j, me] = gbuf[pl.ds(pl.multiple_of((j * GROUP + me) * PITCH, 8), 32), :]

    lax.fori_loop(0, 32, prepare, 0)
    for block in range(4):
        for copy in in_copies[block]:
            copy.wait()
        lax.fori_loop(block * 8, block * 8 + 8, weigh, 0)
        if block == 0:
            table_copies[0].wait()
        transform(0, block)
        if block == 0:
            pl.semaphore_wait(barrier, len(near) + len(others))
            for p, q in beside:
                pl.semaphore_signal(
                    ready_sem, inc=1, device_id={"px": p, "py": q}, device_id_type=MESH
                )
        if block < 3:
            send(near, 0, block * 8, 8)
    pl.semaphore_wait(ready_sem, len(beside))
    send(far, 0, 0, 32)
    send(near, 0, 24, 8)
    keep(0)
    table_copies[1].wait()

    last = CHUNKS - 1

    def message(p, q):
        return gbuf.at[pl.ds(pl.multiple_of((last * GROUP + p * 8 + q) * PITCH, 8), 32), :]

    for block in range(4):
        transform(last, block)
    keep(last)
    for slot, (p, q) in enumerate(shared(1 - core)):
        pltpu.make_async_remote_copy(
            src_ref=message(p, q),
            dst_ref=hbuf.at[slot],
            send_sem=mate_sem.at[0],
            recv_sem=mate_sem.at[1],
            device_id={"sa": mate},
            device_id_type=MESH,
        ).start()

    def forward(j, carry):
        for block in range(4):
            transform(j, block)
        send(peers, j, 0, 32)
        keep(j)
        return carry

    lax.fori_loop(1, last, forward, 0)
    pltpu.make_async_copy(hbuf, hbuf, mate_sem.at[1]).wait()

    def send_last(own):
        def one(slot, p, q):
            pltpu.make_async_remote_copy(
                src_ref=message(p, q) if own else hbuf.at[slot],
                dst_ref=rbuf.at[last, me],
                send_sem=send_sem.at[last],
                recv_sem=recv_sem.at[last],
                device_id={"px": p, "py": q, "sa": sa if own else mate},
                device_id_type=MESH,
            ).start()

        *most, final = shared(core)
        for slot, (p, q) in enumerate(most):
            one(slot, p, q)
        pl.when(core == 1)(lambda: one(len(most), *final))

    @pl.when(core == 0)
    def _():
        send_last(True)
        send_last(False)

    @pl.when(core == 1)
    def _():
        send_last(False)
        send_last(True)

    table_copies[2].wait()
    pltpu.make_async_copy(ty, ty, table_sem.at[3]).wait()

    low_lanes = lax.broadcasted_iota(jnp.int32, (N, 128), 1) < 64

    def finish(j, carry):
        arrived = rbuf.at[j, pl.ds(0, GROUP - 1)]
        pltpu.make_async_copy(arrived, arrived, recv_sem.at[j]).wait()
        for pair in range(2):
            first, second = (
                rbuf[j, pl.ds((pair * 2 + k) * 8, 8)].reshape(N, 128) for k in range(2)
            )
            even = jnp.where(low_lanes, first, pltpu.roll(second, 64, 1))
            odd = jnp.where(low_lanes, pltpu.roll(first, 64, 1), second)
            for k, value in enumerate((even, odd)):
                rows = pl.ds(k * N, N)
                columns = pl.ds(pair * 128, 128)
                high, low = split(value)
                bhigh[rows, columns] = high
                blow[rows, columns] = low
        terms = []
        for odd in range(2):
            rows, above = pl.ds(odd * N, N), odd * 512
            high, low = tz[above : above + N], tz[above + N : above + 2 * N]
            terms.append(
                dot(high, bhigh[rows, :], False)
                + dot(low, bhigh[rows, :], False)
                + dot(high, blow[rows, :], False)
            )
        for upper, value in enumerate((terms[0] + terms[1], terms[0] - terms[1])):
            rows = pl.ds(upper * 128, 128)
            for part in range(2):
                high, low = split(value[part * 128 : part * 128 + 128])
                whigh[rows, pl.ds(part * N, N)] = high
                wlow[rows, pl.ds(part * N, N)] = low
        for half in range(2):
            both = dot(ty[half * N : half * N + N], whigh[...], True)
            field = both[:128] + both[128:] + dot(ty[half * N : half * N + 128], wlow[...], True)
            obuf[j, pl.ds(half * 128, 128), :] = jnp.exp(log_spread * field)
            for place, other in enumerate(others):
                if place // 4 != half:
                    continue
                pltpu.make_async_remote_copy(
                    src_ref=obuf.at[j, pl.ds(place * 32, 32), :],
                    dst_ref=out_ref.at[sa, j],
                    send_sem=out_send_sem.at[j],
                    recv_sem=out_recv_sem.at[j],
                    device_id={"sa": other},
                    device_id_type=MESH,
                ).start()
        out_ref[sa, j] = obuf[j, pl.ds(7 * 32, 32), :]
        return carry

    lax.fori_loop(0, CHUNKS, finish, 0)

    for served in range(2):
        sent = rbuf.at[last, pl.ds(0, 30 + 2 * served)]
        pl.when(core == served)(pltpu.make_async_copy(sent, sent, send_sem.at[last]).wait)
    pltpu.make_async_copy(hbuf, hbuf, mate_sem.at[0]).wait()

    def drain_sent(j, carry):
        sent = rbuf.at[j, pl.ds(0, GROUP - 1)]
        pltpu.make_async_copy(sent, sent, send_sem.at[j]).wait()
        return carry

    lax.fori_loop(0, last, drain_sent, 0)

    def drain(j, carry):
        moved = obuf.at[j, pl.ds(0, 7 * 32), :]
        pltpu.make_async_copy(moved, moved, out_send_sem.at[j]).wait()
        pltpu.make_async_copy(moved, moved, out_recv_sem.at[j]).wait()
        return carry

    lax.fori_loop(0, CHUNKS, drain, 0)


def local(real_coeffs, imaginary_coeffs):
    anywhere = pl.BlockSpec(memory_space=pltpu.HBM)
    spare = np.zeros((2048, N), jnp.bfloat16)
    tables = np.concatenate([x_table(), z_table(), y_table(), spare])
    return pl.pallas_call(
        kernel,
        out_shape=jax.ShapeDtypeStruct((8, CHUNKS, 32, N), jnp.float32),
        in_specs=[anywhere] * 3,
        out_specs=pl.BlockSpec(memory_space=pltpu.VMEM),
        scratch_shapes=[
            pltpu.VMEM((2, 2048, 128), jnp.float32),
            pltpu.VMEM((4, 64, PITCH, 128), jnp.float32),
            pltpu.VMEM((2, 2048, N), jnp.bfloat16),
            pltpu.VMEM((2, 2048, N), jnp.bfloat16),
            pltpu.VMEM((CHUNKS * GROUP * PITCH, 128), jnp.float32),
            pltpu.VMEM((GROUP // 2, 32, 128), jnp.float32),
            pltpu.VMEM((CHUNKS, GROUP, 32, 128), jnp.float32),
            pltpu.VMEM((CHUNKS, N, N), jnp.float32),
            pltpu.VMEM((CHUNKS * 128, N), jnp.bfloat16),
            pltpu.VMEM((1024, N), jnp.bfloat16),
            pltpu.VMEM((512, 512), jnp.bfloat16),
            pltpu.VMEM((N, 512), jnp.bfloat16),
            pltpu.VMEM((N, 512), jnp.bfloat16),
            pltpu.VMEM((512, N), jnp.bfloat16),
            pltpu.VMEM((512, N), jnp.bfloat16),
            pltpu.SemaphoreType.DMA((4, 4)),
            pltpu.SemaphoreType.DMA((4,)),
            pltpu.SemaphoreType.DMA((CHUNKS,)),
            pltpu.SemaphoreType.DMA((CHUNKS,)),
            pltpu.SemaphoreType.DMA((CHUNKS,)),
            pltpu.SemaphoreType.DMA((CHUNKS,)),
            pltpu.SemaphoreType.DMA((2,)),
            pltpu.SemaphoreType.REGULAR,
        ],
        compiler_params=pltpu.CompilerParams(
            collective_id=0, has_side_effects=True, vmem_limit_bytes=50 * 1024 * 1024
        ),
    )(real_coeffs, imaginary_coeffs, tables)


def solution(mesh):
    placed = (P("sa", "px", "py", None), P("sa", "px", "py", None))
    return jax.shard_map(
        local,
        mesh=mesh,
        in_specs=placed,
        out_specs=P(None, ("px", "py"), "sa", None),
        check_vma=False,
    )
```

```python
import math

import jax
import jax.numpy as jnp
import numpy as np
from jax import lax
from jax.experimental import pallas as pl
from jax.experimental.pallas import tpu as pltpu
from jax.sharding import PartitionSpec as P

MESH = pl.DeviceIdType.MESH
corr_length = 1.0
log_spread = 0.5

N = 256
GROUP = 32
CHUNKS = 8
PITCH = 40


def matern(squared, length):
    return 1.0 / (1.0 + (2.0 * math.pi * corr_length / length) ** 2 * squared)


def matern_scale(length):
    middle = length // 2
    square_counts = {}
    for position in range(length):
        square_value = ((position + middle) % length - middle) ** 2
        square_counts[square_value] = square_counts.get(square_value, 0) + 1
    plane_counts = {}
    for first_square, first_count in square_counts.items():
        for second_square, second_count in square_counts.items():
            plane_sum = first_square + second_square
            plane_counts[plane_sum] = plane_counts.get(plane_sum, 0) + first_count * second_count
    running = 0.0
    for first_square, first_count in square_counts.items():
        for plane_sum, plane_count in plane_counts.items():
            running = (
                running + first_count * plane_count * matern(first_square + plane_sum, length) ** 2
            )
    return 1.0 / math.sqrt(running)


def halves(table):
    high = table.astype(np.float32).astype(jnp.bfloat16)
    low = (table - high.astype(np.float64)).astype(np.float32).astype(jnp.bfloat16)
    return high, low


def phases(rows, columns):
    angles = (np.asarray(rows)[:, None] * np.asarray(columns)[None, :] % N) * (2.0 * np.pi / N)
    return np.cos(angles), np.sin(angles)


def x_table():
    pieces = []
    for j in range(CHUNKS):
        cos, sin = phases(np.arange(GROUP) * CHUNKS + j, np.arange(N // 2))
        pieces += halves(np.block([[cos, -sin], [sin, cos]]))
    return np.concatenate(pieces, axis=0)


def z_table():
    owner, block, part, row = np.meshgrid(*(np.arange(n) for n in (8, 4, 2, 4)), indexing="ij")
    real = part.reshape(-1)[None, :] == 0
    pieces = []
    for odd in range(2):
        waves = (owner * 32 + (block * 4 + row) * 2 + odd).reshape(-1)
        cos, sin = phases(np.arange(N // 2), waves)
        pieces += halves(np.concatenate([np.where(real, cos, -sin), np.where(real, sin, cos)]))
    return np.concatenate(pieces, axis=0)


def y_table():
    cos, sin = phases(np.arange(N), np.arange(N))
    return np.concatenate([*halves(cos), *halves(-sin)], axis=0)


def split(value):
    high = value.astype(jnp.bfloat16)
    low = (value - high.astype(jnp.float32)).astype(jnp.bfloat16)
    return high, low


def dot(left, right, transposed):
    return lax.dot_general(
        left,
        right,
        (((1,), (1 if transposed else 0,)), ((), ())),
        preferred_element_type=jnp.float32,
    )


def signed(positions):
    return ((positions + N // 2) % N - N // 2).astype(jnp.float32)


def kernel(
    re_hbm, im_hbm, tables_hbm, out_ref,
    wbuf, xbuf, dhigh, dlow, gbuf, hbuf, rbuf, obuf, tx, tz, ty, whigh, wlow, bhigh, blow,
    in_sem, table_sem, send_sem, recv_sem, out_send_sem, out_recv_sem, mate_sem, ready_sem,
):
    px, py, sa = lax.axis_index("px"), lax.axis_index("py"), lax.axis_index("sa")
    me = px * 8 + py
    z, y = px * 2 + lax.div(py, 4), lax.rem(py, 4)

    in_copies = []
    for block in range(4):
        group = []
        for part, source in enumerate((re_hbm, im_hbm)):
            for half in range(2):
                group.append(
                    pltpu.make_async_copy(
                        source.at[0, :, pl.ds(block * 8, 8), pl.ds(half * 128, 128)],
                        xbuf.at[part * 2 + half, :, pl.ds(block * 8, 8), :],
                        in_sem.at[block, part * 2 + half],
                    )
                )
        in_copies.append(group)
    table_copies = [
        pltpu.make_async_copy(
            tables_hbm.at[pl.ds(start, size), :], target.at[pl.ds(at, size), :], table_sem.at[i]
        )
        for i, (start, size, target, at) in enumerate(
            ((0, 128, tx, 0), (128, 896, tx, 128), (1024, 1024, tz, 0))
        )
    ]
    for copy in in_copies[0]:
        copy.start()
    table_copies[0].start()

    def plane_peer(dz, dy):
        z2, y2 = lax.rem(z + (dz + 8) % 8, 8), lax.rem(y + dy, 4)
        return lax.div(z2, 2), lax.rem(z2, 2) * 4 + y2

    near, far = (
        [plane_peer(dz, dy) for dz in dzs for dy in range(4) if (dz, dy) != (0, 0)]
        for dzs in ((2, -2, 1, -1, 0), (4, 3, -3))
    )
    peers = far + near
    beside = [plane_peer(2, 0), plane_peer(-2, 0)]
    x, core = lax.div(sa, 2), lax.rem(sa, 2)
    mate = x * 2 + (1 - core)
    places = [(dz, dy) for dz in (4, 3, -3, 2, -2, 1, -1, 0) for dy in (1, 0)]

    def shared(of_core):
        return [plane_peer(dz, of_core * 2 + dy) for dz, dy in places]

    others = [
        lax.rem(x + dx, 4) * 2 + lax.rem(core + dc, 2)
        for dx, dc in ((2, 0), (1, 0), (3, 0), (2, 1), (1, 1), (3, 1), (0, 1))
    ]

    barrier = pltpu.get_barrier_semaphore()
    for p, q in near:
        pl.semaphore_signal(barrier, inc=1, device_id={"px": p, "py": q}, device_id_type=MESH)
    for other in others:
        pl.semaphore_signal(barrier, inc=1, device_id={"sa": other}, device_id_type=MESH)

    for group in in_copies[1:]:
        for copy in group:
            copy.start()
    for copy in table_copies[1:]:
        copy.start()
    scale = matern_scale(N)
    slope = (2.0 * math.pi * corr_length / N) ** 2
    fy = signed(lax.broadcasted_iota(jnp.int32, (64, 128), 0) + px * 64) ** 2
    lanes = lax.broadcasted_iota(jnp.int32, (64, 128), 1)
    flat = signed(lanes) ** 2 + fy, signed(lanes + 128) ** 2 + fy
    lines = xbuf.reshape(4, 64 * PITCH, 128)

    def prepare(k, carry):
        fz = signed(py * 32 + k) ** 2
        rows = pl.ds(pl.multiple_of(k * 64, 64), 64)
        for half in range(2):
            wbuf[half, rows, :] = (1.0 / (1.0 + slope * (flat[half] + fz))) * scale
        return carry

    def weigh(k, carry):
        rows = pl.ds(pl.multiple_of(k * 64, 64), 64)
        for part in range(2):
            columns = pl.ds(part * 128, 128)
            first, second = (
                lines[part * 2 + half, pl.ds(k, 64, stride=PITCH), :] * wbuf[half, rows, :]
                for half in range(2)
            )
            for odd, value in enumerate((first + second, first - second)):
                high, low = split(value)
                dhigh[odd, rows, columns] = high
                dlow[odd, rows, columns] = low
        return carry

    def transform(j, block):
        base = j * (GROUP * PITCH)
        table = pl.multiple_of(j * 128, 128)
        odd = j % 2 if isinstance(j, int) else lax.rem(j, 2)
        for piece in range(2):
            rows = pl.ds(block * 512 + piece * 256, 256)
            both = dot(tx[pl.ds(table, 128), :], dhigh[odd, rows, :], True)
            rest = dot(tx[pl.ds(table, 64), :], dlow[odd, rows, :], True)
            result = both[:64] + both[64:] + rest
            for part in range(2):
                for half in range(2):
                    at = base + block * 8 + part * 4 + piece * 2 + half
                    gbuf[pl.ds(at, GROUP, stride=PITCH), :] = result[
                        part * 32 : part * 32 + 32, half * 128 : half * 128 + 128
                    ]

    def send(targets, j, first, count):
        for p, q in targets:
            row = pl.multiple_of((j * GROUP + p * 8 + q) * PITCH + first, 8)
            pltpu.make_async_remote_copy(
                src_ref=gbuf.at[pl.ds(row, count), :],
                dst_ref=rbuf.at[j, me, pl.ds(first, count), :],
                send_sem=send_sem.at[j],
                recv_sem=recv_sem.at[j],
                device_id={"px": p, "py": q},
                device_id_type=MESH,
            ).start()

    def keep(j):
        rbuf[j, me] = gbuf[pl.ds(pl.multiple_of((j * GROUP + me) * PITCH, 8), 32), :]

    lax.fori_loop(0, 32, prepare, 0)
    for block in range(4):
        for copy in in_copies[block]:
            copy.wait()
        lax.fori_loop(block * 8, block * 8 + 8, weigh, 0)
        if block == 0:
            table_copies[0].wait()
        transform(0, block)
        if block == 0:
            pl.semaphore_wait(barrier, len(near) + len(others))
            for p, q in beside:
                pl.semaphore_signal(
                    ready_sem, inc=1, device_id={"px": p, "py": q}, device_id_type=MESH
                )
        if block < 3:
            send(near, 0, block * 8, 8)
        if block == 0:
            for part in range(2):
                for precision in range(2):
                    for place, owner in enumerate([*others, sa]):
                        half, slot = divmod(place, 4)
                        pltpu.make_async_copy(
                            tables_hbm.at[
                                pl.ds(pl.multiple_of(2048 + part * 512 + precision * N + owner * 32, 32), 32), :
                            ],
                            ty.at[pl.ds(half * N + precision * 128 + slot * 32, 32), pl.ds(part * N, N)],
                            table_sem.at[3],
                        ).start()
    pl.semaphore_wait(ready_sem, len(beside))
    send(far, 0, 0, 32)
    send(near, 0, 24, 8)
    keep(0)
    table_copies[1].wait()

    last = CHUNKS - 1

    def message(p, q):
        return gbuf.at[pl.ds(pl.multiple_of((last * GROUP + p * 8 + q) * PITCH, 8), 32), :]

    for block in range(4):
        transform(last, block)
    keep(last)
    for slot, (p, q) in enumerate(shared(1 - core)):
        pltpu.make_async_remote_copy(
            src_ref=message(p, q),
            dst_ref=hbuf.at[slot],
            send_sem=mate_sem.at[0],
            recv_sem=mate_sem.at[1],
            device_id={"sa": mate},
            device_id_type=MESH,
        ).start()

    def forward(j, carry):
        for block in range(4):
            transform(j, block)
        send(peers, j, 0, 32)
        keep(j)
        return carry

    lax.fori_loop(1, last, forward, 0)
    pltpu.make_async_copy(hbuf, hbuf, mate_sem.at[1]).wait()

    def send_last(own):
        def one(slot, p, q):
            pltpu.make_async_remote_copy(
                src_ref=message(p, q) if own else hbuf.at[slot],
                dst_ref=rbuf.at[last, me],
                send_sem=send_sem.at[last],
                recv_sem=recv_sem.at[last],
                device_id={"px": p, "py": q, "sa": sa if own else mate},
                device_id_type=MESH,
            ).start()

        *most, final = shared(core)
        for slot, (p, q) in enumerate(most):
            one(slot, p, q)
        pl.when(core == 1)(lambda: one(len(most), *final))

    @pl.when(core == 0)
    def _():
        send_last(True)
        send_last(False)

    @pl.when(core == 1)
    def _():
        send_last(False)
        send_last(True)

    table_copies[2].wait()
    pltpu.make_async_copy(ty, ty, table_sem.at[3]).wait()

    low_lanes = lax.broadcasted_iota(jnp.int32, (N, 128), 1) < 64

    def finish(j, carry):
        arrived = rbuf.at[j, pl.ds(0, GROUP - 1)]
        pltpu.make_async_copy(arrived, arrived, recv_sem.at[j]).wait()
        for pair in range(2):
            first, second = (
                rbuf[j, pl.ds((pair * 2 + k) * 8, 8)].reshape(N, 128) for k in range(2)
            )
            even = jnp.where(low_lanes, first, pltpu.roll(second, 64, 1))
            odd = jnp.where(low_lanes, pltpu.roll(first, 64, 1), second)
            for k, value in enumerate((even, odd)):
                rows = pl.ds(k * N, N)
                columns = pl.ds(pair * 128, 128)
                high, low = split(value)
                bhigh[rows, columns] = high
                blow[rows, columns] = low
        terms = []
        for odd in range(2):
            rows, above = pl.ds(odd * N, N), odd * 512
            high, low = tz[above : above + N], tz[above + N : above + 2 * N]
            terms.append(
                dot(high, bhigh[rows, :], False)
                + dot(low, bhigh[rows, :], False)
                + dot(high, blow[rows, :], False)
            )
        for upper, value in enumerate((terms[0] + terms[1], terms[0] - terms[1])):
            rows = pl.ds(upper * 128, 128)
            for part in range(2):
                high, low = split(value[part * 128 : part * 128 + 128])
                whigh[rows, pl.ds(part * N, N)] = high
                wlow[rows, pl.ds(part * N, N)] = low
        for half in range(2):
            both = dot(ty[half * N : half * N + N], whigh[...], True)
            field = both[:128] + both[128:] + dot(ty[half * N : half * N + 128], wlow[...], True)
            obuf[j, pl.ds(half * 128, 128), :] = jnp.exp(log_spread * field)
            for place, other in enumerate(others):
                if place // 4 != half:
                    continue
                pltpu.make_async_remote_copy(
                    src_ref=obuf.at[j, pl.ds(place * 32, 32), :],
                    dst_ref=out_ref.at[sa, j],
                    send_sem=out_send_sem.at[j],
                    recv_sem=out_recv_sem.at[j],
                    device_id={"sa": other},
                    device_id_type=MESH,
                ).start()
        out_ref[sa, j] = obuf[j, pl.ds(7 * 32, 32), :]
        return carry

    lax.fori_loop(0, CHUNKS, finish, 0)

    for served in range(2):
        sent = rbuf.at[last, pl.ds(0, 30 + 2 * served)]
        pl.when(core == served)(pltpu.make_async_copy(sent, sent, send_sem.at[last]).wait)
    pltpu.make_async_copy(hbuf, hbuf, mate_sem.at[0]).wait()

    def drain_sent(j, carry):
        sent = rbuf.at[j, pl.ds(0, GROUP - 1)]
        pltpu.make_async_copy(sent, sent, send_sem.at[j]).wait()
        return carry

    lax.fori_loop(0, last, drain_sent, 0)

    def drain(j, carry):
        moved = obuf.at[j, pl.ds(0, 7 * 32), :]
        pltpu.make_async_copy(moved, moved, out_send_sem.at[j]).wait()
        pltpu.make_async_copy(moved, moved, out_recv_sem.at[j]).wait()
        return carry

    lax.fori_loop(0, CHUNKS, drain, 0)


def local(real_coeffs, imaginary_coeffs):
    anywhere = pl.BlockSpec(memory_space=pltpu.HBM)
    spare = np.zeros((2048, N), jnp.bfloat16)
    tables = np.concatenate([x_table(), z_table(), y_table(), spare])
    return pl.pallas_call(
        kernel,
        out_shape=jax.ShapeDtypeStruct((8, CHUNKS, 32, N), jnp.float32),
        in_specs=[anywhere] * 3,
        out_specs=pl.BlockSpec(memory_space=pltpu.VMEM),
        scratch_shapes=[
            pltpu.VMEM((2, 2048, 128), jnp.float32),
            pltpu.VMEM((4, 64, PITCH, 128), jnp.float32),
            pltpu.VMEM((2, 2048, N), jnp.bfloat16),
            pltpu.VMEM((2, 2048, N), jnp.bfloat16),
            pltpu.VMEM((CHUNKS * GROUP * PITCH, 128), jnp.float32),
            pltpu.VMEM((GROUP // 2, 32, 128), jnp.float32),
            pltpu.VMEM((CHUNKS, GROUP, 32, 128), jnp.float32),
            pltpu.VMEM((CHUNKS, N, N), jnp.float32),
            pltpu.VMEM((CHUNKS * 128, N), jnp.bfloat16),
            pltpu.VMEM((1024, N), jnp.bfloat16),
            pltpu.VMEM((512, 512), jnp.bfloat16),
            pltpu.VMEM((N, 512), jnp.bfloat16),
            pltpu.VMEM((N, 512), jnp.bfloat16),
            pltpu.VMEM((512, N), jnp.bfloat16),
            pltpu.VMEM((512, N), jnp.bfloat16),
            pltpu.SemaphoreType.DMA((4, 4)),
            pltpu.SemaphoreType.DMA((4,)),
            pltpu.SemaphoreType.DMA((CHUNKS,)),
            pltpu.SemaphoreType.DMA((CHUNKS,)),
            pltpu.SemaphoreType.DMA((CHUNKS,)),
            pltpu.SemaphoreType.DMA((CHUNKS,)),
            pltpu.SemaphoreType.DMA((2,)),
            pltpu.SemaphoreType.REGULAR,
        ],
        compiler_params=pltpu.CompilerParams(
            collective_id=0, has_side_effects=True, vmem_limit_bytes=50 * 1024 * 1024
        ),
    )(real_coeffs, imaginary_coeffs, tables)


def solution(mesh):
    placed = (P("sa", "px", "py", None), P("sa", "px", "py", None))
    return jax.shard_map(
        local,
        mesh=mesh,
        in_specs=placed,
        out_specs=P(None, ("px", "py"), "sa", None),
        check_vma=False,
    )
```

```python
import math

import jax
import jax.numpy as jnp
import numpy as np
from jax import lax
from jax.experimental import pallas as pl
from jax.experimental.pallas import tpu as pltpu
from jax.sharding import PartitionSpec as P

MESH = pl.DeviceIdType.MESH
corr_length = 1.0
log_spread = 0.5

N = 256
GROUP = 32
CHUNKS = 8
PITCH = 40


def matern(squared, length):
    return 1.0 / (1.0 + (2.0 * math.pi * corr_length / length) ** 2 * squared)


def matern_scale(length):
    middle = length // 2
    square_counts = {}
    for position in range(length):
        square_value = ((position + middle) % length - middle) ** 2
        square_counts[square_value] = square_counts.get(square_value, 0) + 1
    plane_counts = {}
    for first_square, first_count in square_counts.items():
        for second_square, second_count in square_counts.items():
            plane_sum = first_square + second_square
            plane_counts[plane_sum] = plane_counts.get(plane_sum, 0) + first_count * second_count
    running = 0.0
    for first_square, first_count in square_counts.items():
        for plane_sum, plane_count in plane_counts.items():
            running = (
                running + first_count * plane_count * matern(first_square + plane_sum, length) ** 2
            )
    return 1.0 / math.sqrt(running)


def halves(table):
    high = table.astype(np.float32).astype(jnp.bfloat16)
    low = (table - high.astype(np.float64)).astype(np.float32).astype(jnp.bfloat16)
    return high, low


def phases(rows, columns):
    angles = (np.asarray(rows)[:, None] * np.asarray(columns)[None, :] % N) * (2.0 * np.pi / N)
    return np.cos(angles), np.sin(angles)


def x_table():
    pieces = []
    for j in range(CHUNKS):
        cos, sin = phases(np.arange(GROUP) * CHUNKS + j, np.arange(N // 2))
        pieces += halves(np.block([[cos, -sin], [sin, cos]]))
    return np.concatenate(pieces, axis=0)


def z_table():
    owner, block, part, row = np.meshgrid(*(np.arange(n) for n in (8, 4, 2, 4)), indexing="ij")
    real = part.reshape(-1)[None, :] == 0
    pieces = []
    for odd in range(2):
        waves = (owner * 32 + (block * 4 + row) * 2 + odd).reshape(-1)
        cos, sin = phases(np.arange(N // 2), waves)
        pieces += halves(np.concatenate([np.where(real, cos, -sin), np.where(real, sin, cos)]))
    return np.concatenate(pieces, axis=0)


def y_table():
    cos, sin = phases(np.arange(N), np.arange(N))
    return np.concatenate([*halves(cos), *halves(-sin)], axis=0)


def split(value):
    high = value.astype(jnp.bfloat16)
    low = (value - high.astype(jnp.float32)).astype(jnp.bfloat16)
    return high, low


def dot(left, right, transposed):
    return lax.dot_general(
        left,
        right,
        (((1,), (1 if transposed else 0,)), ((), ())),
        preferred_element_type=jnp.float32,
    )


def signed(positions):
    return ((positions + N // 2) % N - N // 2).astype(jnp.float32)


def kernel(
    re_hbm, im_hbm, tables_hbm, out_ref,
    wbuf, xbuf, dhigh, dlow, gbuf, hbuf, rbuf, obuf, tx, tz, ty, whigh, wlow, bhigh, blow,
    in_sem, table_sem, send_sem, recv_sem, out_send_sem, out_recv_sem, mate_sem, ready_sem,
):
    px, py, sa = lax.axis_index("px"), lax.axis_index("py"), lax.axis_index("sa")
    me = px * 8 + py
    z, y = px * 2 + lax.div(py, 4), lax.rem(py, 4)

    in_copies = []
    for block in range(4):
        group = []
        for part, source in enumerate((re_hbm, im_hbm)):
            for half in range(2):
                group.append(
                    pltpu.make_async_copy(
                        source.at[0, :, pl.ds(block * 8, 8), pl.ds(half * 128, 128)],
                        xbuf.at[part * 2 + half, :, pl.ds(block * 8, 8), :],
                        in_sem.at[block, part * 2 + half],
                    )
                )
        in_copies.append(group)
    table_copies = [
        pltpu.make_async_copy(
            tables_hbm.at[pl.ds(start, size), :], target.at[pl.ds(at, size), :], table_sem.at[i]
        )
        for i, (start, size, target, at) in enumerate(
            ((0, 128, tx, 0), (128, 896, tx, 128), (1024, 1024, tz, 0))
        )
    ]
    for copy in in_copies[0]:
        copy.start()
    table_copies[0].start()

    def plane_peer(dz, dy):
        z2, y2 = lax.rem(z + (dz + 8) % 8, 8), lax.rem(y + dy, 4)
        return lax.div(z2, 2), lax.rem(z2, 2) * 4 + y2

    near, far = (
        [plane_peer(dz, dy) for dz in dzs for dy in range(4) if (dz, dy) != (0, 0)]
        for dzs in ((2, -2, 1, -1, 0), (4, 3, -3))
    )
    peers = far + near
    beside = [plane_peer(2, 0), plane_peer(-2, 0)]
    x, core = lax.div(sa, 2), lax.rem(sa, 2)
    mate = x * 2 + (1 - core)
    places = [(dz, dy) for dz in (4, 3, -3, 2, -2, 1, -1, 0) for dy in (1, 0)]

    def shared(of_core):
        return [plane_peer(dz, of_core * 2 + dy) for dz, dy in places]

    others = [
        lax.rem(x + dx, 4) * 2 + lax.rem(core + dc, 2)
        for dx, dc in ((2, 0), (1, 0), (3, 0), (2, 1), (1, 1), (3, 1), (0, 1))
    ]

    barrier = pltpu.get_barrier_semaphore()
    for p, q in near:
        pl.semaphore_signal(barrier, inc=1, device_id={"px": p, "py": q}, device_id_type=MESH)
    for other in others:
        pl.semaphore_signal(barrier, inc=1, device_id={"sa": other}, device_id_type=MESH)

    for group in in_copies[1:]:
        for copy in group:
            copy.start()
    for copy in table_copies[1:]:
        copy.start()
    scale = matern_scale(N)
    slope = (2.0 * math.pi * corr_length / N) ** 2
    fy = signed(lax.broadcasted_iota(jnp.int32, (64, 128), 0) + px * 64) ** 2
    lanes = lax.broadcasted_iota(jnp.int32, (64, 128), 1)
    flat = signed(lanes) ** 2 + fy, signed(lanes + 128) ** 2 + fy
    lines = xbuf.reshape(4, 64 * PITCH, 128)

    def prepare(k, carry):
        fz = signed(py * 32 + k) ** 2
        rows = pl.ds(pl.multiple_of(k * 64, 64), 64)
        for half in range(2):
            wbuf[half, rows, :] = (1.0 / (1.0 + slope * (flat[half] + fz))) * scale
        return carry

    def weigh(k, carry):
        rows = pl.ds(pl.multiple_of(k * 64, 64), 64)
        for part in range(2):
            columns = pl.ds(part * 128, 128)
            first, second = (
                lines[part * 2 + half, pl.ds(k, 64, stride=PITCH), :] * wbuf[half, rows, :]
                for half in range(2)
            )
            for odd, value in enumerate((first + second, first - second)):
                high, low = split(value)
                dhigh[odd, rows, columns] = high
                dlow[odd, rows, columns] = low
        return carry

    def transform(j, block):
        base = j * (GROUP * PITCH)
        table = pl.multiple_of(j * 128, 128)
        odd = j % 2 if isinstance(j, int) else lax.rem(j, 2)
        for piece in range(2):
            rows = pl.ds(block * 512 + piece * 256, 256)
            both = dot(tx[pl.ds(table, 128), :], dhigh[odd, rows, :], True)
            rest = dot(tx[pl.ds(table, 64), :], dlow[odd, rows, :], True)
            result = both[:64] + both[64:] + rest
            for part in range(2):
                for half in range(2):
                    at = base + block * 8 + part * 4 + piece * 2 + half
                    gbuf[pl.ds(at, GROUP, stride=PITCH), :] = result[
                        part * 32 : part * 32 + 32, half * 128 : half * 128 + 128
                    ]

    def send(targets, j, first, count):
        for p, q in targets:
            row = pl.multiple_of((j * GROUP + p * 8 + q) * PITCH + first, 8)
            pltpu.make_async_remote_copy(
                src_ref=gbuf.at[pl.ds(row, count), :],
                dst_ref=rbuf.at[j, me, pl.ds(first, count), :],
                send_sem=send_sem.at[j],
                recv_sem=recv_sem.at[j],
                device_id={"px": p, "py": q},
                device_id_type=MESH,
            ).start()

    def keep(j):
        rbuf[j, me] = gbuf[pl.ds(pl.multiple_of((j * GROUP + me) * PITCH, 8), 32), :]

    lax.fori_loop(0, 32, prepare, 0)
    for block in range(4):
        for copy in in_copies[block]:
            copy.wait()
        lax.fori_loop(block * 8, block * 8 + 8, weigh, 0)
        if block == 0:
            table_copies[0].wait()
        transform(0, block)
        if block == 0:
            pl.semaphore_wait(barrier, len(near) + len(others))
            for p, q in beside:
                pl.semaphore_signal(
                    ready_sem, inc=1, device_id={"px": p, "py": q}, device_id_type=MESH
                )
        send(near, 0, block * 8, 8)
        if block == 0:
            for part in range(2):
                for precision in range(2):
                    for place, owner in enumerate([*others, sa]):
                        half, slot = divmod(place, 4)
                        pltpu.make_async_copy(
                            tables_hbm.at[
                                pl.ds(pl.multiple_of(2048 + part * 512 + precision * N + owner * 32, 32), 32), :
                            ],
                            ty.at[pl.ds(half * N + precision * 128 + slot * 32, 32), pl.ds(part * N, N)],
                            table_sem.at[3],
                        ).start()
    pl.semaphore_wait(ready_sem, len(beside))
    send(far, 0, 0, 32)
    keep(0)
    table_copies[1].wait()

    last = CHUNKS - 1

    def message(p, q):
        return gbuf.at[pl.ds(pl.multiple_of((last * GROUP + p * 8 + q) * PITCH, 8), 32), :]

    for block in range(4):
        transform(last, block)
    keep(last)
    for slot, (p, q) in enumerate(shared(1 - core)):
        pltpu.make_async_remote_copy(
            src_ref=message(p, q),
            dst_ref=hbuf.at[slot],
            send_sem=mate_sem.at[0],
            recv_sem=mate_sem.at[1],
            device_id={"sa": mate},
            device_id_type=MESH,
        ).start()

    def forward(j, carry):
        for block in range(4):
            transform(j, block)
        send(peers, j, 0, 32)
        keep(j)
        return carry

    lax.fori_loop(1, last, forward, 0)
    pltpu.make_async_copy(hbuf, hbuf, mate_sem.at[1]).wait()

    def send_last(own):
        def one(slot, p, q):
            pltpu.make_async_remote_copy(
                src_ref=message(p, q) if own else hbuf.at[slot],
                dst_ref=rbuf.at[last, me],
                send_sem=send_sem.at[last],
                recv_sem=recv_sem.at[last],
                device_id={"px": p, "py": q, "sa": sa if own else mate},
                device_id_type=MESH,
            ).start()

        *most, final = shared(core)
        for slot, (p, q) in enumerate(most):
            one(slot, p, q)
        pl.when(core == 1)(lambda: one(len(most), *final))

    @pl.when(core == 0)
    def _():
        send_last(True)
        send_last(False)

    @pl.when(core == 1)
    def _():
        send_last(False)
        send_last(True)

    table_copies[2].wait()
    pltpu.make_async_copy(ty, ty, table_sem.at[3]).wait()

    low_lanes = lax.broadcasted_iota(jnp.int32, (N, 128), 1) < 64

    def finish(j, carry):
        arrived = rbuf.at[j, pl.ds(0, GROUP - 1)]
        pltpu.make_async_copy(arrived, arrived, recv_sem.at[j]).wait()
        for pair in range(2):
            first, second = (
                rbuf[j, pl.ds((pair * 2 + k) * 8, 8)].reshape(N, 128) for k in range(2)
            )
            even = jnp.where(low_lanes, first, pltpu.roll(second, 64, 1))
            odd = jnp.where(low_lanes, pltpu.roll(first, 64, 1), second)
            for k, value in enumerate((even, odd)):
                rows = pl.ds(k * N, N)
                columns = pl.ds(pair * 128, 128)
                high, low = split(value)
                bhigh[rows, columns] = high
                blow[rows, columns] = low
        terms = []
        for odd in range(2):
            rows, above = pl.ds(odd * N, N), odd * 512
            high, low = tz[above : above + N], tz[above + N : above + 2 * N]
            terms.append(
                dot(high, bhigh[rows, :], False)
                + dot(low, bhigh[rows, :], False)
                + dot(high, blow[rows, :], False)
            )
        for upper, value in enumerate((terms[0] + terms[1], terms[0] - terms[1])):
            rows = pl.ds(upper * 128, 128)
            for part in range(2):
                high, low = split(value[part * 128 : part * 128 + 128])
                whigh[rows, pl.ds(part * N, N)] = high
                wlow[rows, pl.ds(part * N, N)] = low
        for half in range(2):
            both = dot(ty[half * N : half * N + N], whigh[...], True)
            field = both[:128] + both[128:] + dot(ty[half * N : half * N + 128], wlow[...], True)
            obuf[j, pl.ds(half * 128, 128), :] = jnp.exp(log_spread * field)
            for place, other in enumerate(others):
                if place // 4 != half:
                    continue
                pltpu.make_async_remote_copy(
                    src_ref=obuf.at[j, pl.ds(place * 32, 32), :],
                    dst_ref=out_ref.at[sa, j],
                    send_sem=out_send_sem.at[j],
                    recv_sem=out_recv_sem.at[j],
                    device_id={"sa": other},
                    device_id_type=MESH,
                ).start()
        out_ref[sa, j] = obuf[j, pl.ds(7 * 32, 32), :]
        return carry

    lax.fori_loop(0, CHUNKS, finish, 0)

    for served in range(2):
        sent = rbuf.at[last, pl.ds(0, 30 + 2 * served)]
        pl.when(core == served)(pltpu.make_async_copy(sent, sent, send_sem.at[last]).wait)
    pltpu.make_async_copy(hbuf, hbuf, mate_sem.at[0]).wait()

    def drain_sent(j, carry):
        sent = rbuf.at[j, pl.ds(0, GROUP - 1)]
        pltpu.make_async_copy(sent, sent, send_sem.at[j]).wait()
        return carry

    lax.fori_loop(0, last, drain_sent, 0)

    def drain(j, carry):
        moved = obuf.at[j, pl.ds(0, 7 * 32), :]
        pltpu.make_async_copy(moved, moved, out_send_sem.at[j]).wait()
        pltpu.make_async_copy(moved, moved, out_recv_sem.at[j]).wait()
        return carry

    lax.fori_loop(0, CHUNKS, drain, 0)


def local(real_coeffs, imaginary_coeffs):
    anywhere = pl.BlockSpec(memory_space=pltpu.HBM)
    spare = np.zeros((2048, N), jnp.bfloat16)
    tables = np.concatenate([x_table(), z_table(), y_table(), spare])
    return pl.pallas_call(
        kernel,
        out_shape=jax.ShapeDtypeStruct((8, CHUNKS, 32, N), jnp.float32),
        in_specs=[anywhere] * 3,
        out_specs=pl.BlockSpec(memory_space=pltpu.VMEM),
        scratch_shapes=[
            pltpu.VMEM((2, 2048, 128), jnp.float32),
            pltpu.VMEM((4, 64, PITCH, 128), jnp.float32),
            pltpu.VMEM((2, 2048, N), jnp.bfloat16),
            pltpu.VMEM((2, 2048, N), jnp.bfloat16),
            pltpu.VMEM((CHUNKS * GROUP * PITCH, 128), jnp.float32),
            pltpu.VMEM((GROUP // 2, 32, 128), jnp.float32),
            pltpu.VMEM((CHUNKS, GROUP, 32, 128), jnp.float32),
            pltpu.VMEM((CHUNKS, N, N), jnp.float32),
            pltpu.VMEM((CHUNKS * 128, N), jnp.bfloat16),
            pltpu.VMEM((1024, N), jnp.bfloat16),
            pltpu.VMEM((512, 512), jnp.bfloat16),
            pltpu.VMEM((N, 512), jnp.bfloat16),
            pltpu.VMEM((N, 512), jnp.bfloat16),
            pltpu.VMEM((512, N), jnp.bfloat16),
            pltpu.VMEM((512, N), jnp.bfloat16),
            pltpu.SemaphoreType.DMA((4, 4)),
            pltpu.SemaphoreType.DMA((4,)),
            pltpu.SemaphoreType.DMA((CHUNKS,)),
            pltpu.SemaphoreType.DMA((CHUNKS,)),
            pltpu.SemaphoreType.DMA((CHUNKS,)),
            pltpu.SemaphoreType.DMA((CHUNKS,)),
            pltpu.SemaphoreType.DMA((2,)),
            pltpu.SemaphoreType.REGULAR,
        ],
        compiler_params=pltpu.CompilerParams(
            collective_id=0, has_side_effects=True, vmem_limit_bytes=50 * 1024 * 1024
        ),
    )(real_coeffs, imaginary_coeffs, tables)


def solution(mesh):
    placed = (P("sa", "px", "py", None), P("sa", "px", "py", None))
    return jax.shard_map(
        local,
        mesh=mesh,
        in_specs=placed,
        out_specs=P(None, ("px", "py"), "sa", None),
        check_vma=False,
    )
```
